256 devices in a mesh: img: 16 (over x, z_lo, core), tp: 16 (over y, z_hi).
Axes of the slice: x: 4, y: 4, z: 8 (z_hi: 4, z_lo: 2; z = z_hi * 2 + z_lo), core: 2. Of those that a mesh axis runs over, the one named last changes fastest.
Arguments:
- patch_tokens: bfloat16 [32768, 1024], P(('img', 'tp')), may hold values from -12 to 12
- norm_gain: float32 [1024], replicated, may hold values from 0.1 to 1.9
- norm_bias: float32 [1024], replicated, may hold values from -3 to 3
- up_weight: bfloat16 [1024, 8192], P('img', 'tp'), may hold values from -0.1875 to 0.1875
- up_bias: float32 [8192], P('tp'), may hold values from -3 to 3
- down_weight: bfloat16 [8192, 4096], P('tp', 'img'), may hold values from -0.125 to 0.125
- down_bias: float32 [4096], replicated, may hold values from -3 to 3
Outputs:
- projected: bfloat16 [32768, 4096], P(('img', 'tp'))
The draws below stay inside these ranges and needn't reach their ends.
All inputs are finite; a program needn't handle non-finite values.
Results may differ from the reference program's by a relative error of at most 0.014.
Values may be sent and summed in bfloat16 or wider, within the bound.
A program may use at most 128 MiB of HBM per device.

```python
import jax
import jax.numpy as jnp
from jax import lax

D = 1024
FF = 8192
DOUT = 4096
TOK_DEV = 128
TOKENS = 32768
N_IMG = 16
N_TP = 16


def level_of(own_key, dims, pieces, low, top_value):
    loudness = 1.0
    for axis_at, blocks in pieces:
        draws = jax.random.uniform(jax.random.fold_in(jax.random.fold_in(own_key, 6), axis_at), (blocks,), jnp.float32, low / len(pieces), top_value / len(pieces))
        loudness = loudness * jnp.repeat(jnp.exp(draws), dims[axis_at] // blocks).reshape((-1,) + (1,) * (len(dims) - 1 - axis_at))
    return loudness


def centred(rng, dims, width, reach, pieces=(), held_as=jnp.bfloat16):
    result = width * jax.random.normal(rng, dims, jnp.float32)
    if pieces:
        result = result * level_of(rng, dims, pieces, -0.22, 0.18)
    return jnp.clip(result, -reach, reach).astype(held_as)


def setup_inputs(seed: int = 0) -> dict:
    keys = jax.random.split(jax.random.key(seed), 8)
    patch_tokens = centred(keys[0], (TOKENS, D), 2.0, 12.0, ((0, 256),))
    norm_gain = jnp.clip(1.0 + 0.18 * jax.random.normal(keys[1], (D,), jnp.float32), 0.1, 1.9)
    norm_bias = centred(keys[2], (D,), 0.5, 3.0, (), jnp.float32)
    up_weight = centred(keys[3], (D, FF), D ** -0.5, 0.1875, ((0, 16), (1, 16)))
    up_bias = centred(keys[4], (FF,), 0.5, 3.0, ((0, 16),), jnp.float32)
    down_weight = centred(keys[5], (FF, DOUT), (FF // 4) ** -0.5, 0.125, ((0, 16), (1, 16)))
    down_bias = centred(keys[6], (DOUT,), 0.5, 3.0, (), jnp.float32)
    return dict(patch_tokens=patch_tokens, norm_gain=norm_gain, norm_bias=norm_bias, up_weight=up_weight, up_bias=up_bias, down_weight=down_weight, down_bias=down_bias)


def normalize(rows, norm_gain, norm_bias):
    values = rows.astype(jnp.float32)
    center = lax.optimization_barrier(jnp.mean(values, axis=1, keepdims=True))
    spread = lax.optimization_barrier(jnp.mean((values - center) ** 2, axis=1, keepdims=True))
    return ((values - center) * lax.rsqrt(spread + 1e-05) * norm_gain + norm_bias).astype(jnp.bfloat16)

def reference(patch_tokens, norm_gain, norm_bias, up_weight, up_bias, down_weight, down_bias):
    block_rows = TOK_DEV * N_TP
    group_width = FF // N_TP
    blocks = patch_tokens.reshape(N_IMG, block_rows, D)

    def one_block(rows):
        normed = normalize(rows, norm_gain, norm_bias)
        hidden = jax.nn.gelu(jnp.dot(normed, up_weight, preferred_element_type=jnp.float32) + up_bias).astype(jnp.bfloat16)

        def add_group(group, total):
            start = (group * group_width).astype(jnp.int32)
            cols = lax.dynamic_slice_in_dim(hidden, start, group_width, 1)
            weights = lax.dynamic_slice_in_dim(down_weight, start, group_width, 0)
            partial_value = jnp.dot(cols, weights, preferred_element_type=jnp.float32).astype(jnp.bfloat16)
            partial_value = lax.optimization_barrier(partial_value)
            return total + partial_value.astype(jnp.float32)
        total = lax.fori_loop(0, N_TP, add_group, jnp.zeros((block_rows, DOUT), jnp.float32))
        return (total + down_bias).astype(jnp.bfloat16)
    return lax.map(one_block, blocks).reshape(TOKENS, DOUT)
```

```python
import jax
import jax.numpy as jnp
from jax import lax
from jax.experimental import pallas as pl
from jax.experimental.pallas import tpu as pltpu
from jax.sharding import PartitionSpec as P

MESH = pl.DeviceIdType.MESH
F32, BF16 = jnp.float32, jnp.bfloat16

WAIT, SEND, SHARE_U, SHARE_D, NORM, HIDDEN, PART, RELAY, FINAL = range(9)
XP, XQ, YP, YQ, ZP, ZQ = range(6)
WU, D0, D1, TOK, SIB_U, SIB_D, FAR, NEAR_P, NEAR_Q = range(9)

STEPS = (
    (SEND, YP, TOK, 0), (SEND, YQ, TOK, 0), (SEND, XP, WU, 0, 0), (SEND, XQ, WU, 0, 0), (SEND, ZP, WU, 0, 0),
    (SEND, ZQ, WU, 0, 0), (SEND, XP, D0, 0, 0), (SEND, XQ, D0, 0, 0), (SEND, ZP, D0, 0, 0), (SEND, ZQ, D0, 0, 0),
    (WAIT, WU, -1, 0), (SEND, XP, WU, -1, 0), (WAIT, WU, 1, 0), (WAIT, WU, 0, -1), (SEND, XQ, WU, 0, -1),
    (SEND, ZP, WU, 0, -1), (SEND, XP, WU, 0, -1), (SEND, ZP, D1, 0, 0), (WAIT, WU, 0, 1), (SEND, ZQ, WU, 0, 1),
    (SEND, XQ, WU, 0, 1), (SEND, ZQ, D1, 0, 0), (SEND, XP, WU, 0, 1), (SEND, XQ, D1, 0, 0), (WAIT, D0, -1, 0),
    (WAIT, D0, 1, 0), (WAIT, D0, 0, -1), (WAIT, D0, 0, 1), (WAIT, WU, 2, 0), (WAIT, WU, 1, -1), (WAIT, TOK, -1),
    (SEND, YP, TOK, -1), (WAIT, TOK, 1), (WAIT, WU, 0, -2), (SEND, XP, WU, 0, -2), (SEND, ZP, WU, 0, -2),
    (SEND, XQ, WU, 0, -2), (SEND, ZP, D0, 0, -1), (WAIT, WU, 0, 2), (SEND, ZQ, WU, 0, 2), (SEND, XP, WU, 0, 2),
    (SEND, ZQ, D0, 0, 1), (SEND, XQ, WU, 0, 2), (SHARE_U, 0), (WAIT, WU, -1, -1), (SEND, XP, WU, -1, -1),
    (WAIT, WU, 1, 1), (WAIT, SIB_U, 0), (WAIT, WU, -1, 1), (SEND, XP, WU, -1, 1), (WAIT, D1, 0, -1),
    (WAIT, D1, 0, 1), (SEND, ZQ, D1, 0, 1), (WAIT, WU, -1, -2), (SEND, XP, WU, -1, -2), (WAIT, D1, 1, 0),
    (WAIT, WU, 0, -3), (SEND, XQ, WU, 0, -3), (SEND, ZP, WU, 0, -3), (SEND, ZP, D1, 0, -1), (SEND, XP, WU, 0, -3),
    (WAIT, WU, 0, 3), (SEND, XQ, WU, 0, 3), (SEND, XQ, D1, 0, -1), (SEND, XP, WU, 0, 3), (WAIT, TOK, 2), (NORM,),
    (WAIT, WU, -1, 2), (SEND, XP, WU, -1, 2), (WAIT, WU, 1, -2), (WAIT, WU, 2, -1), (WAIT, WU, 1, 2),
    (WAIT, D0, 0, -2), (SEND, ZP, D0, 0, -2), (WAIT, D0, 0, 2), (SEND, ZQ, D0, 0, 2), (SHARE_U, -1),
    (WAIT, WU, 2, 1), (WAIT, WU, 1, -3), (WAIT, WU, 0, -4), (SEND, XQ, WU, 0, -4), (SEND, XP, WU, 0, -4),
    (SEND, XQ, D1, 0, 1), (SHARE_U, 1), (WAIT, SIB_U, 1), (WAIT, WU, 2, -2), (WAIT, WU, 1, 3), (WAIT, D1, 0, 2),
    (SEND, ZQ, D1, 0, 2), (SEND, ZQ, D0, -1, 0), (SEND, XQ, D1, 0, 2), (SEND, ZQ, D0, 1, 0), (SHARE_U, -2),
    (WAIT, SIB_U, -1), (WAIT, WU, -1, -3), (SEND, XP, WU, -1, -3), (WAIT, D1, 0, -2), (SEND, ZP, D1, 0, -2),
    (SEND, XQ, D1, 0, -2), (WAIT, SIB_U, 2), (WAIT, WU, -1, 3), (SEND, XP, WU, -1, 3), (WAIT, D1, 1, -1),
    (WAIT, D0, 0, 3), (WAIT, WU, 2, 2), (WAIT, WU, 1, -4), (WAIT, D0, 0, -3), (SEND, ZP, D0, 0, -3), (SHARE_U, 2),
    (SHARE_D, 0, 0, 1), (WAIT, WU, -1, -4), (SEND, XP, WU, -1, -4), (SEND, XP, D0, -1, 0), (SEND, XP, D1, 0, 0),
    (SEND, XP, D1, 0, -1), (SEND, XP, D1, 0, 1), (SEND, XP, D1, 0, 2), (SEND, XP, D1, 0, -2), (WAIT, D1, 0, 3),
    (SEND, XQ, D1, 0, 3), (SEND, XP, D1, 0, 3), (WAIT, SIB_U, -2), (WAIT, WU, 2, -3), (WAIT, D1, 1, 1),
    (WAIT, D1, 0, -3), (SEND, ZP, D1, 0, -3), (SEND, ZP, D0, -1, 0), (SEND, XQ, D1, 0, -3), (SEND, ZP, D0, 1, 0),
    (SEND, XP, D1, 0, -3), (WAIT, SIB_D, 0, 0, 1), (SHARE_U, -3), (SHARE_D, 1, 0, 1), (WAIT, WU, 2, 3),
    (WAIT, D0, -1, 1), (SEND, ZQ, D0, -1, 1), (SHARE_U, 3), (WAIT, SIB_U, 3), (WAIT, WU, 2, -4), (WAIT, D1, 1, 2),
    (WAIT, D0, 0, -4), (WAIT, SIB_D, 1, 0, 1), (SHARE_U, -4), (SHARE_D, 0, 0, 0), (WAIT, SIB_U, -3),
    (WAIT, D0, 1, 1), (SEND, ZQ, D0, 1, 1), (WAIT, SIB_U, -4), (HIDDEN,), (WAIT, D0, 2, 0), (SEND, ZP, D0, 2, 0),
    (SEND, ZQ, D0, 2, 0), (WAIT, D1, 1, -2), (WAIT, D1, 0, -4), (SEND, XQ, D1, 0, -4), (SEND, XP, D1, 0, -4),
    (WAIT, SIB_D, 0, 0, 0), (WAIT, D0, -1, 2), (SEND, ZQ, D0, -1, 2), (WAIT, D1, -1, 0), (SEND, XP, D1, -1, 0),
    (WAIT, D1, 1, 3), (WAIT, D0, -1, -1), (SEND, ZP, D0, -1, -1), (SHARE_D, 1, 0, 0), (PART, 0, 0, 0),
    (WAIT, D0, 1, 2), (SEND, ZQ, D0, 1, 2), (WAIT, D0, 1, -1), (SEND, ZP, D0, 1, -1), (PART, 0, 0, 1),
    (WAIT, D1, -1, -1), (SEND, XP, D1, -1, -1), (WAIT, D1, 1, -3), (WAIT, SIB_D, 1, 0, 0), (SHARE_D, 1, 1, 1),
    (PART, 1, 0, 0), (PART, 1, 0, 1), (WAIT, D1, -1, 1), (SEND, XP, D1, -1, 1), (WAIT, D0, 2, -1), (WAIT, D0, 2, 1),
    (SEND, ZQ, D0, 2, 1), (WAIT, FAR, 0, 0, 0), (WAIT, NEAR_P, 0, 0, 0), (WAIT, D1, 1, -4), (WAIT, SIB_D, 1, -1, 1),
    (SHARE_D, 1, 1, 0), (RELAY, 0, 0, 0), (WAIT, D1, -1, 2), (SEND, XP, D1, -1, 2), (WAIT, FAR, 0, 0, 1),
    (WAIT, NEAR_P, 0, 0, 1), (RELAY, 0, 0, 1), (WAIT, D1, -1, -2), (SEND, XP, D1, -1, -2), (WAIT, SIB_D, 1, -1, 0),
    (WAIT, D0, -1, -2), (SEND, ZP, D0, -1, -2), (SEND, ZP, D0, 2, -1), (WAIT, D0, -1, 3), (WAIT, FAR, 1, 0, 0),
    (WAIT, NEAR_P, 1, 0, 0), (RELAY, 1, 0, 0), (WAIT, D1, -1, 3), (SEND, XP, D1, -1, 3), (WAIT, FAR, 1, 0, 1),
    (WAIT, NEAR_P, 1, 0, 1), (RELAY, 1, 0, 1), (WAIT, NEAR_Q, 0, 0, 0), (FINAL, 0, 0, 0), (WAIT, D1, -1, -3),
    (SEND, XP, D1, -1, -3), (SHARE_D, 1, -1, 1), (PART, 1, -1, 1), (WAIT, D0, 1, -2), (SEND, ZP, D0, 1, -2),
    (WAIT, D0, 1, 3), (WAIT, NEAR_Q, 0, 0, 1), (WAIT, NEAR_Q, 1, 0, 0), (FINAL, 0, 0, 1), (WAIT, D1, -1, -4),
    (SEND, XP, D1, -1, -4), (SHARE_D, 1, -1, 0), (PART, 1, -1, 0), (WAIT, NEAR_Q, 1, 0, 1), (WAIT, SIB_D, 1, 1, 1),
    (WAIT, D1, 2, 0), (PART, 1, 1, 1), (WAIT, D0, -1, -3), (SEND, ZP, D0, -1, -3), (WAIT, D0, 2, 2),
    (SEND, ZQ, D0, 2, 2), (WAIT, SIB_D, 1, 1, 0), (SHARE_D, 0, -1, 1), (PART, 1, 1, 0), (WAIT, D1, 2, -1),
    (WAIT, D0, 2, -2), (WAIT, FAR, 1, -1, 1), (WAIT, NEAR_P, 1, -1, 1), (RELAY, 1, -1, 1), (FINAL, 1, 0, 0),
    (WAIT, D1, 2, 1), (FINAL, 1, 0, 1), (WAIT, D0, 1, -3), (SEND, ZP, D0, 1, -3), (SEND, ZP, D0, 2, -2),
    (SHARE_D, 0, 1, 1), (WAIT, FAR, 1, -1, 0), (WAIT, NEAR_P, 1, -1, 0), (RELAY, 1, -1, 0), (WAIT, SIB_D, 0, 1, 1),
    (PART, 0, 1, 1), (WAIT, D1, 2, 2), (WAIT, FAR, 1, 1, 1), (WAIT, NEAR_P, 1, 1, 1), (RELAY, 1, 1, 1),
    (WAIT, SIB_D, 0, -1, 1), (PART, 0, -1, 1), (WAIT, D1, 2, -2), (WAIT, D0, -1, -4), (WAIT, D0, 2, 3),
    (WAIT, FAR, 1, 1, 0), (WAIT, NEAR_P, 1, 1, 0), (SHARE_D, 0, -1, 0), (RELAY, 1, 1, 0), (WAIT, NEAR_Q, 1, -1, 1),
    (WAIT, D1, 2, 3), (FINAL, 1, -1, 1), (WAIT, D0, 1, -4), (SHARE_D, 0, 1, 0), (WAIT, NEAR_P, 0, 1, 1),
    (WAIT, NEAR_Q, 1, -1, 0), (FINAL, 1, -1, 0), (WAIT, D1, 2, -3), (SHARE_D, 1, 2, 1), (WAIT, D0, 2, -3),
    (SEND, ZP, D0, 2, -3), (SHARE_D, 0, 2, 1), (WAIT, SIB_D, 0, 1, 0), (PART, 0, 1, 0), (WAIT, FAR, 0, 1, 1),
    (WAIT, D1, 2, -4), (WAIT, NEAR_P, 0, -1, 1), (WAIT, SIB_D, 0, -1, 0), (WAIT, NEAR_Q, 1, 1, 1),
    (SHARE_D, 1, 2, 0), (RELAY, 0, 1, 1), (PART, 0, -1, 0), (WAIT, FAR, 0, -1, 1), (WAIT, SIB_D, 1, 2, 1),
    (WAIT, NEAR_Q, 1, 1, 0), (RELAY, 0, -1, 1), (PART, 1, 2, 1), (WAIT, SIB_D, 0, 2, 1), (WAIT, D0, 2, -4),
    (WAIT, SIB_D, 1, 2, 0), (SHARE_D, 0, 2, 0), (PART, 0, 2, 1), (WAIT, FAR, 0, 1, 0), (WAIT, NEAR_P, 0, 1, 0),
    (RELAY, 0, 1, 0), (PART, 1, 2, 0), (WAIT, NEAR_Q, 0, 1, 1), (WAIT, NEAR_P, 0, -1, 0), (WAIT, SIB_D, 0, 2, 0),
    (PART, 0, 2, 0), (WAIT, FAR, 0, -1, 0), (WAIT, NEAR_P, 1, 2, 1), (RELAY, 0, -1, 0), (FINAL, 0, 1, 1),
    (FINAL, 1, 1, 0), (FINAL, 1, 1, 1), (WAIT, NEAR_Q, 0, -1, 1), (FINAL, 0, -1, 1), (WAIT, NEAR_P, 0, 2, 1),
    (WAIT, FAR, 1, 2, 1), (RELAY, 1, 2, 1), (WAIT, NEAR_P, 1, 2, 0), (WAIT, FAR, 0, 2, 1), (RELAY, 0, 2, 1),
    (WAIT, NEAR_P, 0, 2, 0), (WAIT, NEAR_Q, 0, 1, 0), (FINAL, 0, 1, 0), (WAIT, FAR, 1, 2, 0), (RELAY, 1, 2, 0),
    (WAIT, FAR, 0, 2, 0), (RELAY, 0, 2, 0), (WAIT, NEAR_Q, 0, -1, 0), (FINAL, 0, -1, 0), (WAIT, NEAR_Q, 1, 2, 1),
    (FINAL, 1, 2, 1), (WAIT, NEAR_Q, 0, 2, 1), (FINAL, 0, 2, 1), (WAIT, NEAR_Q, 1, 2, 0), (FINAL, 1, 2, 0),
    (WAIT, NEAR_Q, 0, 2, 0), (FINAL, 0, 2, 0),
)

KINDS = (WU, D0, D1)
ITEMS = [(h, dx, rp) for h in (0, 1) for dx in (0, -1, 1, 2) for rp in (0, 1)]
OFFSETS = (0, -1, 1, -2, 2, -3, 3, -4)
AFTER = {XP: -1, XQ: 1, YP: -1, YQ: 1, ZP: -1, ZQ: 1}


def slot(dx):
    return dx % 4


def piece_index(kind, dx, dz):
    return KINDS.index(kind) * 32 + slot(dx) * 8 + dz % 8


def kernel(
    tok, gain, nbias, up, upb, down, dbias, out,
    X, N, U, UB, D, H, A0, A1, S1, S2, S3, RL, FP, FQ,
    loc, wsend, wrecv, xsend, xrecv, bsend, brecv, sibs, sibr, ysend, yrecv,
):
    img, tp = lax.axis_index("img"), lax.axis_index("tp")
    c = lax.rem(img, 2)
    zlo = lax.rem(img // 2, 2)
    x = img // 4
    zhi = lax.rem(tp, 4)
    y = tp // 4
    z = zhi * 2 + zlo
    sign = 1 - 2 * c

    def wrap(v, n):
        return lax.rem(v + 2 * n, n)

    def at(dx=0, dy=0, dz=0, core=None):
        xx, yy, zz = wrap(x + sign * dx, 4), wrap(y + sign * dy, 4), wrap(z + sign * dz, 8)
        cc = c if core is None else core
        return {"img": xx * 4 + lax.rem(zz, 2) * 2 + cc, "tp": yy * 4 + zz // 2}

    sibling = at(core=1 - c)
    link = {
        XP: at(dx=1), XQ: at(dx=-1), YP: at(dy=1), YQ: at(dy=-1), ZP: at(dz=1), ZQ: at(dz=-1),
    }
    far = (at(dz=2), at(dz=-2), at(dz=4))

    copies = [
        pltpu.make_async_copy(tok, X.at[0], loc.at[0]),
        pltpu.make_async_copy(up, U.at[zhi, x, zlo, c], loc.at[1]),
        pltpu.make_async_copy(down.at[:, pl.ds(0, 128)], D.at[0, 0, 0, zhi, :, pl.ds(0, 128)], loc.at[2]),
        pltpu.make_async_copy(down.at[:, pl.ds(128, 128)], D.at[1, 0, 0, zhi, :, pl.ds(0, 128)], loc.at[3]),
        pltpu.make_async_copy(upb, UB.at[zhi], loc.at[4]),
    ]
    for copy in copies:
        copy.start()
    barrier = pltpu.get_barrier_semaphore()
    partners = [sibling, *link.values(), *far]
    for device in partners:
        pl.semaphore_signal(barrier, inc=1, device_id=device, device_id_type=MESH)
    pl.semaphore_wait(barrier, len(partners))
    for copy in copies:
        copy.wait()

    sends = []

    def send(src, dst, ssem, rsem, device):
        copy = pltpu.make_async_remote_copy(
            src_ref=src, dst_ref=dst, send_sem=ssem, recv_sem=rsem, device_id=device, device_id_type=MESH
        )
        copy.start()
        sends.append(copy)

    def arrive(ref, rsem):
        pltpu.make_async_remote_copy(
            src_ref=ref, dst_ref=ref, send_sem=rsem, recv_sem=rsem, device_id=sibling, device_id_type=MESH
        ).wait_recv()

    def where(kind, dx, dz):
        zz = wrap(z + sign * dz, 8)
        if kind == WU:
            return U.at[zz // 2, wrap(x + sign * dx, 4), lax.rem(zz, 2), c]
        return D.at[kind - D0, slot(dx), dz % 2, zz // 2, :, pl.ds(0, 128)]

    def place(kind, dx, dz, dx_there, dz_there):
        if kind == WU:
            return where(kind, dx, dz)
        zz = wrap(z + sign * dz, 8)
        return D.at[kind - D0, slot(dx_there), dz_there % 2, zz // 2, :, pl.ds(0, 128)]

    used = [0, 0]

    def forward(path, kind, dx, dz):
        step = AFTER[path]
        dx_there, dz_there = (dx + step, dz) if path in (XP, XQ) else (dx, dz + step)
        send(
            where(kind, dx, dz),
            place(kind, dx, dz, dx_there, dz_there),
            wsend.at[used[0]],
            wrecv.at[piece_index(kind, dx_there, dz_there)],
            link[path],
        )
        used[0] += 1

    def forward_tokens(path, dy):
        there = slot(dy + AFTER[path])
        send(X.at[slot(dy)], X.at[there], xsend.at[there - 1], xrecv.at[there - 1], link[path])

    def send_y(src, dst, rsem, device):
        send(src, dst, ysend.at[used[1]], rsem, device)
        used[1] += 1

    for i, device in enumerate(far):
        send(UB.at[zhi], UB.at[zhi], bsend.at[i], brecv.at[i], device)

    for step in STEPS:
        op, args = step[0], step[1:]
        if op == SEND:
            if args[1] == TOK:
                forward_tokens(args[0], args[2])
            else:
                forward(*args)
        elif op == WAIT:
            kind = args[0]
            if kind == TOK:
                arrive(X.at[slot(args[1])], xrecv.at[slot(args[1]) - 1])
            elif kind in KINDS:
                arrive(where(*args), wrecv.at[piece_index(*args)])
            elif kind == SIB_U:
                zz = wrap(z + sign * args[1], 8)
                arrive(U.at[zz // 2, :, lax.rem(zz, 2), 1 - c], sibr.at[16 + args[1] % 8])
            elif kind == SIB_D:
                h, dx, rp = args[1:]
                arrive(D.at[h, slot(dx), rp, :, :, pl.ds(128, 128)], sibr.at[ITEMS.index((h, dx, rp))])
            else:
                i = ITEMS.index(args[1:])
                buffer, base = {FAR: (RL, 0), NEAR_P: (FP, 16), NEAR_Q: (FQ, 32)}[kind]
                arrive(buffer.at[i], yrecv.at[base + i])
        elif op == SHARE_U:
            dz = args[0]
            zz = wrap(z + sign * dz, 8)
            block = U.at[zz // 2, :, lax.rem(zz, 2), c]
            send(block, block, sibs.at[16 + dz % 8], sibr.at[16 + (-dz) % 8], sibling)
        elif op == SHARE_D:
            h, dx, rp = args
            i, there = ITEMS.index(args), ITEMS.index((h, -dx if dx in (-1, 1) else dx, rp))
            send(
                D.at[h, slot(dx), rp, :, :, pl.ds(0, 128)],
                D.at[h, slot(-dx), rp, :, :, pl.ds(128, 128)],
                sibs.at[i],
                sibr.at[there],
                sibling,
            )
        elif op == NORM:

            @pl.loop(0, 4)
            def _(r):
                values = X[r].astype(F32)
                center = jnp.mean(values, axis=1, keepdims=True)
                spread = jnp.mean((values - center) ** 2, axis=1, keepdims=True)
                rows = (values - center) * lax.rsqrt(spread + 1e-05) * gain[...] + nbias[...]
                N[pl.ds(pl.multiple_of(r * 128, 128), 128), :] = rows.astype(BF16)

        elif op == HIDDEN:
            for i in range(3):
                zz = wrap(z + sign * (-2, 2, 4)[i], 8)
                arrive(UB.at[zz // 2], brecv.at[i])

            @pl.loop(0, 4)
            def _(g):
                summed = jnp.dot(N[...], U[g].reshape(1024, 512), preferred_element_type=F32)
                hidden = jax.nn.gelu(summed + UB[g], approximate=True)
                H[:, pl.ds(pl.multiple_of(g * 512, 512), 512)] = hidden.astype(BF16)

        elif op == PART:
            h, dx, rp = args
            i = ITEMS.index(args)
            part = jnp.dot(H[...], D[h, slot(dx), rp].reshape(2048, 256), preferred_element_type=F32)
            S2[i] = part[256:384].astype(BF16)
            send_y(S2.at[i], RL.at[i], yrecv.at[i], link[YP])
            S3[i] = part[384:512].astype(BF16)
            send_y(S3.at[i], FP.at[i], yrecv.at[16 + i], link[YQ])
            A0[i] = part[0:128]
            A1[i] = part[128:256]
        elif op == RELAY:
            i = ITEMS.index(args)
            S1[i] = (A1[i] + RL[i].astype(F32)).astype(BF16)
            send_y(S1.at[i], FQ.at[i], yrecv.at[32 + i], link[YP])
        elif op == FINAL:
            h, dx, rp = args
            i = ITEMS.index(args)
            block = wrap(x + sign * dx, 4) * 4 + lax.rem(zlo + rp, 2) * 2
            total = A0[i] + FP[i].astype(F32) + FQ[i].astype(F32)
            for half, core in ((0, c), (1, 1 - c)):
                cols = pl.ds(pl.multiple_of((block + core) * 256 + h * 128, 128), 128)
                out[:, cols] = (total[:, half * 128 : half * 128 + 128] + dbias[:, cols]).astype(BF16)

    for copy in sends:
        copy.wait_send()


def on_device(patch_tokens, norm_gain, norm_bias, up_weight, up_bias, down_weight, down_bias):
    hbm = pl.BlockSpec(memory_space=pl.ANY)
    vmem = pl.BlockSpec(memory_space=pltpu.VMEM)
    dma = pltpu.SemaphoreType.DMA
    return pl.pallas_call(
        kernel,
        out_shape=jax.ShapeDtypeStruct((128, 4096), BF16),
        in_specs=[hbm, vmem, vmem, hbm, hbm, hbm, vmem],
        out_specs=vmem,
        scratch_shapes=[
            pltpu.VMEM((4, 128, 1024), BF16),
            pltpu.VMEM((512, 1024), BF16),
            pltpu.VMEM((4, 4, 2, 2, 64, 512), BF16),
            pltpu.VMEM((4, 1, 512), F32),
            pltpu.VMEM((2, 4, 2, 4, 512, 256), BF16),
            pltpu.VMEM((512, 2048), BF16),
            pltpu.VMEM((16, 128, 256), F32),
            pltpu.VMEM((16, 128, 256), F32),
            *[pltpu.VMEM((16, 128, 256), BF16)] * 6,
            dma((5,)),
            dma((93,)),
            dma((96,)),
            dma((3,)),
            dma((3,)),
            dma((3,)),
            dma((3,)),
            dma((24,)),
            dma((24,)),
            dma((48,)),
            dma((48,)),
        ],
        compiler_params=pltpu.CompilerParams(
            collective_id=0, has_side_effects=True, vmem_limit_bytes=62 * 1024 * 1024
        ),
    )(
        patch_tokens,
        norm_gain.reshape(1, -1),
        norm_bias.reshape(1, -1),
        up_weight,
        up_bias.reshape(1, -1),
        down_weight,
        down_bias.reshape(1, -1),
    )


def solution(mesh):
    return jax.shard_map(
        on_device,
        mesh=mesh,
        in_specs=(P(("img", "tp"), None), P(), P(), P("img", "tp"), P("tp"), P("tp", "img"), P()),
        out_specs=P(("img", "tp"), None),
        check_vma=False,
    )
```

```python
import jax
import jax.numpy as jnp
from jax import lax
from jax.experimental import pallas as pl
from jax.experimental.pallas import tpu as pltpu
from jax.sharding import PartitionSpec as P

MESH = pl.DeviceIdType.MESH
F32, BF16 = jnp.float32, jnp.bfloat16

WAIT, SEND, SHARE_U, SHARE_D, NORM, HIDDEN, PART, DIRECT, RELAY, FINAL, LAST = range(11)
XP, XQ, YP, YQ, ZP, ZQ = range(6)
TOK, SIB_U, SIB_D, FAR = range(-4, 0)

WU, D0, D1 = range(3)
PIECES = ((None, 0, 64), (0, 0, 512), (1, 0, 512))
BIASED = WU
FROM_X = (D0,)

STEPS = (
    (SEND, XP, WU, 0, 0), (SEND, XQ, WU, 0, 0), (SEND, YP, TOK, 0), (SEND, YQ, TOK, 0), (SEND, ZP, WU, 0, 0),
    (SEND, ZQ, WU, 0, 0), (SEND, XP, D0, 0, 0), (SEND, XQ, D0, 0, 0), (SEND, ZP, D1, 0, 0), (SEND, ZQ, D1, 0, 0),
    (WAIT, WU, -1, 0), (WAIT, WU, 0, -1), (SEND, XP, WU, 0, -1), (SEND, XQ, WU, 0, -1), (SEND, ZP, WU, 0, -1),
    (SEND, ZP, D0, 0, 0), (WAIT, WU, 0, 1), (SEND, ZQ, WU, 0, 1), (SEND, XP, WU, 0, 1), (SEND, XQ, WU, 0, 1),
    (SEND, ZQ, D0, 0, 0), (SEND, XP, WU, -1, 0), (SEND, XQ, D1, 0, 0), (WAIT, D0, -1, 0), (WAIT, D0, 1, 0),
    (WAIT, D1, 0, -1), (SEND, ZP, D1, 0, -1), (WAIT, D1, 0, 1), (SEND, ZQ, D1, 0, 1), (WAIT, WU, -1, -1),
    (WAIT, TOK, -1), (SEND, YP, TOK, -1), (WAIT, TOK, 1), (WAIT, WU, 0, -2), (SEND, XP, WU, 0, -2),
    (SEND, XQ, WU, 0, -2), (SEND, ZP, WU, 0, -2), (WAIT, WU, 0, 2), (SEND, XP, WU, 0, 2), (SEND, XP, WU, -1, -1),
    (SEND, XQ, WU, 0, 2), (SEND, ZQ, WU, 0, 2), (SEND, XQ, D1, 0, -1), (WAIT, WU, -1, 1), (WAIT, D0, 0, -1),
    (SEND, ZP, D0, 0, -1), (WAIT, D0, 0, 1), (SEND, ZQ, D0, 0, 1), (SHARE_U, 0), (WAIT, WU, -1, -2),
    (SEND, XP, WU, -1, -2), (SEND, XP, WU, -1, 1), (WAIT, SIB_U, 0), (WAIT, TOK, 2), (NORM,), (WAIT, WU, -1, 2),
    (WAIT, D1, 0, -2), (SEND, ZP, D1, 0, -2), (WAIT, D1, 0, 2), (SEND, ZQ, D1, 0, 2), (WAIT, WU, 0, -3),
    (SEND, XP, WU, 0, -3), (SEND, XQ, WU, 0, -3), (SEND, ZP, WU, 0, -3), (WAIT, WU, 0, 3), (SEND, XP, WU, 0, 3),
    (SEND, XQ, WU, 0, 3), (SEND, XP, WU, -1, 2), (SEND, XQ, D1, 0, -2), (SEND, XQ, D1, 0, 2), (SHARE_U, -1),
    (SHARE_U, -2), (WAIT, SIB_U, 1), (WAIT, D0, 0, -2), (SEND, ZP, D0, 0, -2), (WAIT, D0, 0, 2),
    (SEND, ZQ, D0, 0, 2), (SEND, ZQ, D0, -1, 0), (SEND, ZQ, D0, 1, 0), (SHARE_U, 1), (WAIT, SIB_U, 2),
    (WAIT, WU, -1, -3), (SEND, XP, WU, -1, -3), (WAIT, SIB_U, -1), (HIDDEN, 0), (WAIT, WU, -1, 3),
    (SEND, XP, WU, -1, 3), (WAIT, D1, 0, -3), (SEND, ZP, D1, 0, -3), (WAIT, D1, 0, 3), (SHARE_D, 1, 0, 1),
    (WAIT, WU, 0, -4), (SEND, XP, WU, 0, -4), (SEND, XP, D0, -1, 0), (SEND, XQ, WU, 0, -4), (SEND, XQ, D1, 0, 1),
    (SHARE_U, 2), (WAIT, SIB_D, 1, 0, 1), (WAIT, D0, 0, 3), (SHARE_U, -3), (WAIT, SIB_U, -2), (HIDDEN, 1),
    (WAIT, D0, 0, -3), (SEND, ZP, D0, 0, -3), (SEND, ZP, D0, -1, 0), (SHARE_U, 3), (SHARE_D, 0, 0, 1),
    (WAIT, SIB_U, 3), (WAIT, WU, -1, -4), (SEND, XP, WU, -1, -4), (SEND, XP, D1, 0, 0), (SEND, XP, D1, 0, -2),
    (SEND, XP, D1, 0, 2), (WAIT, D0, -1, 1), (SEND, ZQ, D0, -1, 1), (WAIT, SIB_U, -3), (HIDDEN, 2),
    (WAIT, D1, 0, -4), (SEND, XQ, D1, 0, -4), (SEND, XQ, D1, 0, -3), (SEND, XQ, D1, 0, 3), (SEND, XP, D1, 0, -4),
    (SEND, XP, D1, 0, -1), (SEND, XP, D1, 0, 1), (SEND, XP, D1, 0, -3), (SEND, XP, D1, 0, 3), (WAIT, SIB_D, 0, 0, 1),
    (SHARE_D, 1, 0, 0), (WAIT, D0, 2, 0), (SEND, ZQ, D0, 2, 0), (SEND, ZP, D0, 2, 0), (WAIT, D0, 1, 1),
    (SEND, ZQ, D0, 1, 1), (WAIT, D0, 0, -4), (WAIT, SIB_D, 1, 0, 0), (SHARE_U, -4), (SHARE_D, 0, 0, 0),
    (WAIT, D0, -1, 2), (SEND, ZQ, D0, -1, 2), (WAIT, SIB_U, -4), (HIDDEN, 3), (WAIT, D1, -1, 0),
    (SEND, XP, D1, -1, 0), (WAIT, D0, -1, -1), (SEND, ZP, D0, -1, -1), (WAIT, SIB_D, 0, 0, 0), (SHARE_D, 1, 1, 0),
    (PART, 0, 0, 1), (PART, 1, 0, 0), (WAIT, D0, 2, 1), (SEND, ZQ, D0, 2, 1), (PART, 1, 0, 1), (WAIT, D1, -1, -2),
    (SEND, XP, D1, -1, -2), (WAIT, D0, 2, -1), (SEND, ZP, D0, 2, -1), (WAIT, SIB_D, 1, -1, 0), (PART, 0, 0, 0),
    (WAIT, D0, 1, 2), (SEND, ZQ, D0, 1, 2), (WAIT, FAR, 0, 0, 1), (RELAY, 0, 0, 1), (WAIT, D1, -1, 2),
    (SEND, XP, D1, -1, 2), (WAIT, D0, -1, -2), (SEND, ZP, D0, -1, -2), (SHARE_D, 1, 1, 1), (WAIT, FAR, 1, 0, 0),
    (RELAY, 1, 0, 0), (WAIT, D1, -1, -4), (SEND, XP, D1, -1, -4), (WAIT, D0, -1, 3), (SHARE_D, 1, -1, 0),
    (PART, 1, -1, 0), (WAIT, FAR, 1, 0, 1), (RELAY, 1, 0, 1), (WAIT, SIB_D, 1, -1, 1), (WAIT, D1, -1, -1),
    (SEND, XP, D1, -1, -1), (WAIT, D0, 2, -2), (SEND, ZP, D0, 2, -2), (WAIT, FAR, 0, 0, 0), (RELAY, 0, 0, 0),
    (WAIT, SIB_D, 1, 1, 0), (PART, 1, 1, 0), (WAIT, D1, -1, 1), (SEND, XP, D1, -1, 1), (WAIT, D0, 2, 2),
    (SEND, ZQ, D0, 2, 2), (FINAL, 0, 0, 1), (FINAL, 1, 0, 0), (WAIT, D1, -1, -3), (SEND, XP, D1, -1, -3),
    (WAIT, D0, -1, -3), (SEND, ZP, D0, -1, -3), (SEND, ZP, D0, 1, 0), (SHARE_D, 0, -1, 1), (WAIT, FAR, 1, -1, 0),
    (RELAY, 1, -1, 0), (WAIT, D1, -1, 3), (SEND, XP, D1, -1, 3), (WAIT, D0, 1, 3), (SHARE_D, 1, -1, 1),
    (PART, 1, -1, 1), (FINAL, 1, 0, 1), (WAIT, SIB_D, 0, 1, 1), (WAIT, D0, 2, -3), (SEND, ZP, D0, 2, -3),
    (FINAL, 0, 0, 0), (WAIT, FAR, 1, 1, 0), (RELAY, 1, 1, 0), (WAIT, SIB_D, 1, 1, 1), (PART, 1, 1, 1),
    (WAIT, D0, 2, 3), (SHARE_D, 0, 2, 1), (FINAL, 1, -1, 0), (WAIT, D0, -1, -4), (SHARE_D, 0, -1, 0),
    (WAIT, FAR, 1, -1, 1), (RELAY, 1, -1, 1), (WAIT, D0, 1, -1), (SEND, ZP, D0, 1, -1), (SHARE_D, 1, 2, 0),
    (FINAL, 1, 1, 0), (WAIT, SIB_D, 0, 2, 1), (PART, 0, 2, 1), (WAIT, D0, 2, -4), (SHARE_D, 0, 2, 0),
    (WAIT, SIB_D, 0, 1, 0), (WAIT, FAR, 1, 1, 1), (RELAY, 1, 1, 1), (WAIT, SIB_D, 1, 2, 0), (PART, 1, 2, 0),
    (WAIT, D0, 1, -2), (SEND, ZP, D0, 1, -2), (FINAL, 1, -1, 1), (WAIT, SIB_D, 0, 2, 0), (PART, 0, 2, 0),
    (WAIT, FAR, 0, 2, 1), (RELAY, 0, 2, 1), (FINAL, 1, 1, 1), (SHARE_D, 1, 2, 1), (WAIT, FAR, 1, 2, 0),
    (WAIT, D0, 1, -3), (SEND, ZP, D0, 1, -3), (SHARE_D, 0, 1, 1), (RELAY, 1, 2, 0), (PART, 0, 1, 1),
    (WAIT, SIB_D, 1, 2, 1), (PART, 1, 2, 1), (WAIT, FAR, 0, 2, 0), (RELAY, 0, 2, 0), (FINAL, 0, 2, 1),
    (WAIT, SIB_D, 0, -1, 1), (PART, 0, -1, 1), (FINAL, 1, 2, 0), (WAIT, D0, 1, -4), (SHARE_D, 0, 1, 0),
    (PART, 0, 1, 0), (WAIT, FAR, 0, 1, 1), (RELAY, 0, 1, 1), (WAIT, FAR, 1, 2, 1), (WAIT, SIB_D, 0, -1, 0),
    (RELAY, 1, 2, 1), (DIRECT, 0, -1, 0), (FINAL, 0, 2, 0), (WAIT, FAR, 0, -1, 1), (RELAY, 0, -1, 1),
    (WAIT, FAR, 0, 1, 0), (RELAY, 0, 1, 0), (FINAL, 0, 1, 1), (FINAL, 1, 2, 1), (LAST, 0, -1, 0), (FINAL, 0, -1, 1),
    (FINAL, 0, 1, 0),
)

ITEMS = [(h, dx, rp) for h in (0, 1) for dx in (0, -1, 1, 2) for rp in (0, 1)]
OFFSETS = (0, -1, 1, -2, 2, -3, 3, -4)
AFTER = {XP: -1, XQ: 1, YP: -1, YQ: 1, ZP: -1, ZQ: 1}


def slot(dx):
    return dx % 4


def piece_index(kind, dx, dz):
    if kind in FROM_X or slot(dx) in (0, 3):
        return kind * 32 + slot(dx) * 8 + dz % 8
    if PIECES[kind][0] is None:
        return kind * 32 + 8 + dz % 8
    return kind * 32 + slot(dx) * 8 + dz % 2


def piece_semaphore(kind, dx, dz):
    return ARRIVALS.index(piece_index(kind, dx, dz))


ARRIVALS = sorted({piece_index(k, dx, dz) for k in range(len(PIECES)) for dx in (0, -1, 1, 2) for dz in OFFSETS if dx or dz})


def kernel(
    tok, gain, nbias, up, upb, down, dbias, out,
    X, N, U, UB, D, H, O, A0, A1, S1, S2, S3, RL, FP, FQ,
    loc, wsend, wrecv, xsend, xrecv, bsend, brecv, sibs, sibr, ysend, yrecv, stored,
):
    img, tp = lax.axis_index("img"), lax.axis_index("tp")
    c = lax.rem(img, 2)
    zlo = lax.rem(img // 2, 2)
    x = img // 4
    zhi = lax.rem(tp, 4)
    y = tp // 4
    z = zhi * 2 + zlo
    sign = 1 - 2 * c

    def wrap(v, n):
        return lax.rem(v + 2 * n, n)

    def at(dx=0, dy=0, dz=0, core=None):
        xx, yy, zz = wrap(x + sign * dx, 4), wrap(y + sign * dy, 4), wrap(z + sign * dz, 8)
        cc = c if core is None else core
        return {"img": xx * 4 + lax.rem(zz, 2) * 2 + cc, "tp": yy * 4 + zz // 2}

    sibling = at(core=1 - c)
    opposite = at(dy=2)
    link = {
        XP: at(dx=1), XQ: at(dx=-1), YP: at(dy=1), YQ: at(dy=-1), ZP: at(dz=1), ZQ: at(dz=-1),
    }

    copies = [
        pltpu.make_async_copy(tok, X.at[0], loc.at[0]),
        pltpu.make_async_copy(up, U.at[zhi, x, zlo, c], loc.at[1]),
        pltpu.make_async_copy(down.at[:, pl.ds(0, 128)], D.at[0, 0, 0, zhi, :, pl.ds(0, 128)], loc.at[2]),
        pltpu.make_async_copy(down.at[:, pl.ds(128, 128)], D.at[1, 0, 0, zhi, :, pl.ds(0, 128)], loc.at[3]),
        pltpu.make_async_copy(upb, UB.at[z], loc.at[4]),
    ]
    for copy in copies:
        copy.start()
    barrier = pltpu.get_barrier_semaphore()
    partners = [sibling, *link.values(), opposite]
    for device in partners:
        pl.semaphore_signal(barrier, inc=1, device_id=device, device_id_type=MESH)
    pl.semaphore_wait(barrier, len(partners))
    for copy in copies:
        copy.wait()

    def send(src, dst, ssem, rsem, device):
        pltpu.make_async_remote_copy(
            src_ref=src, dst_ref=dst, send_sem=ssem, recv_sem=rsem, device_id=device, device_id_type=MESH
        ).start()

    def arrive(ref, rsem):
        pltpu.make_async_remote_copy(
            src_ref=ref, dst_ref=ref, send_sem=rsem, recv_sem=rsem, device_id=sibling, device_id_type=MESH
        ).wait_recv()

    def where(kind, dx, dz, dx_there=None, dz_there=None):
        half, row, rows = PIECES[kind]
        zz = wrap(z + sign * dz, 8)
        if half is None:
            return U.at[zz // 2, wrap(x + sign * dx, 4), lax.rem(zz, 2), c, pl.ds(row, rows)]
        dx_there = dx if dx_there is None else dx_there
        dz_there = dz if dz_there is None else dz_there
        return D.at[half, slot(dx_there), dz_there % 2, zz // 2, pl.ds(row, rows), pl.ds(0, 128)]

    def some(kind, power):
        half, _, rows = PIECES[kind]
        if half is None:
            whole = U.at[:, :, :, :, pl.ds(0, rows)]
            return (whole.at[0, 0, 0, 0], whole.at[0, 0, 0], whole.at[0, 0], whole.at[0, 0:2], whole.at[0])[power]
        whole = D.at[:, :, :, :, pl.ds(0, rows), pl.ds(0, 128)]
        return (whole.at[0, 0, 0, 0], whole.at[0, 0, 0, 0:2], whole.at[0, 0, 0], whole.at[0, 0], whole.at[0, 0:2])[power]

    sent = [0] * len(PIECES)
    used = [0]

    def forward(path, kind, dx, dz):
        step = AFTER[path]
        dx_there, dz_there = (dx + step, dz) if path in (XP, XQ) else (dx, dz + step)
        send(
            where(kind, dx, dz),
            where(kind, dx, dz, dx_there, dz_there),
            wsend.at[kind * 5 + (sent[kind] + 1).bit_length() - 1],
            wrecv.at[piece_semaphore(kind, dx_there, dz_there)],
            link[path],
        )
        sent[kind] += 1
        if kind == BIASED and path in (ZP, ZQ):
            bias = UB.at[wrap(z + sign * dz, 8)]
            send(bias, bias, bsend.at[0], brecv.at[dz_there % 8], link[path])

    def forward_tokens(path, dy):
        there = slot(dy + AFTER[path])
        send(X.at[slot(dy)], X.at[there], xsend.at[0], xrecv.at[there - 1], link[path])

    def send_y(src, dst, rsem, device):
        send(src, dst, ysend.at[used[0] // 16], rsem, device)
        used[0] += 1

    for step in STEPS:
        op, args = step[0], step[1:]
        if op == SEND:
            if args[1] == TOK:
                forward_tokens(args[0], args[2])
            else:
                forward(*args)
        elif op == WAIT:
            kind = args[0]
            if kind == TOK:
                arrive(X.at[slot(args[1])], xrecv.at[slot(args[1]) - 1])
            elif kind >= 0:
                arrive(where(*args), wrecv.at[piece_semaphore(*args)])
                if kind == BIASED and args[1] == 0:
                    arrive(UB.at[wrap(z + sign * args[2], 8)], brecv.at[args[2] % 8])
            elif kind == SIB_U:
                zz = wrap(z + sign * args[1], 8)
                arrive(U.at[zz // 2, :, lax.rem(zz, 2), 1 - c], sibr.at[16 + args[1] % 8])
            elif kind == SIB_D:
                h, dx, rp = args[1:]
                arrive(D.at[h, slot(dx), rp, :, :, pl.ds(128, 128)], sibr.at[ITEMS.index((h, dx, rp))])
            else:
                i = ITEMS.index(args[1:])
                arrive(RL.at[i], yrecv.at[i])
        elif op == SHARE_U:
            dz = args[0]
            zz = wrap(z + sign * dz, 8)
            block = U.at[zz // 2, :, lax.rem(zz, 2), c]
            for kind, (half, _, _) in enumerate(PIECES):
                if half is None and kind not in FROM_X:
                    arrive(some(kind, 1), wrecv.at[piece_semaphore(kind, 1, dz)])
            send(block, block, sibs.at[1], sibr.at[16 + (-dz) % 8], sibling)
        elif op == SHARE_D:
            h, dx, rp = args
            there = ITEMS.index((h, -dx if dx in (-1, 1) else dx, rp))
            for kind, (half, _, _) in enumerate(PIECES):
                if half == h and kind not in FROM_X and dx in (1, 2):
                    arrive(some(kind, 2), wrecv.at[piece_semaphore(kind, dx, rp)])
            send(
                D.at[h, slot(dx), rp, :, :, pl.ds(0, 128)],
                D.at[h, slot(-dx), rp, :, :, pl.ds(128, 128)],
                sibs.at[0],
                sibr.at[there],
                sibling,
            )
        elif op == NORM:

            @pl.loop(0, 4)
            def _(r):
                values = X[r].astype(F32)
                center = jnp.mean(values, axis=1, keepdims=True)
                spread = jnp.mean((values - center) ** 2, axis=1, keepdims=True)
                rows = (values - center) * lax.rsqrt(spread + 1e-05) * gain[...] + nbias[...]
                N[pl.ds(pl.multiple_of(r * 128, 128), 128), :] = rows.astype(BF16)

        elif op == HIDDEN:
            side = 1 - 2 * zlo
            zz = wrap(z + (0, -2 * side, 2 * side, 4)[args[0]], 8)
            g = zz // 2
            summed = jnp.dot(N[...], U[g].reshape(1024, 512), preferred_element_type=F32)
            hidden = jax.nn.gelu(summed + UB[zz], approximate=True)
            H[:, pl.ds(pl.multiple_of(g * 512, 512), 512)] = hidden.astype(BF16)

        elif op in (PART, DIRECT):
            h, dx, rp = args
            i = ITEMS.index(args)
            columns = D[h, slot(dx), rp].reshape(2048, 256)
            here, there = (jnp.dot(H[m : m + 256], columns, preferred_element_type=F32) for m in (0, 256))
            A0[i] = here[0:128]
            S2[i] = there[0:128].astype(BF16)
            S3[i] = there[128:256].astype(BF16)
            if op == PART:
                A1[i] = here[128:256]
                send_y(S2.at[i], RL.at[i], yrecv.at[i], link[YP])
                send_y(S3.at[i], FP.at[i], yrecv.at[16 + i], link[YQ])
            else:
                S1[i] = here[128:256].astype(BF16)
                send_y(S2.at[i], RL.at[i], yrecv.at[16 + i], opposite)
                send_y(S3.at[i], FP.at[i], yrecv.at[16 + i], link[YQ])
                send_y(S1.at[i], FQ.at[i], yrecv.at[16 + i], link[YP])
        elif op == RELAY:
            i = ITEMS.index(args)
            S1[i] = (A1[i] + RL[i].astype(F32)).astype(BF16)
            send_y(S1.at[i], FQ.at[i], yrecv.at[16 + i], link[YP])
        elif op in (FINAL, LAST):
            h, dx, rp = args
            i = ITEMS.index(args)
            block = wrap(x + sign * dx, 4) * 4 + lax.rem(zlo + rp, 2) * 2
            arrive(FP.at[0 : 2 if op == FINAL else 3], yrecv.at[16 + i])
            total = A0[i] + FP[i].astype(F32) + FQ[i].astype(F32)
            if op == LAST:
                total = total + RL[i].astype(F32)
            for half, core in ((0, c), (1, 1 - c)):
                cols = pl.ds(pl.multiple_of((block + core) * 256 + h * 128, 128), 128)
                O[:, cols] = (total[:, half * 128 : half * 128 + 128] + dbias[:, cols]).astype(BF16)
                pltpu.make_async_copy(O.at[:, cols], out.at[:, cols], stored.at[0]).start()

    def left(ref, ssem):
        pltpu.make_async_remote_copy(
            src_ref=ref, dst_ref=ref, send_sem=ssem, recv_sem=ssem, device_id=sibling, device_id_type=MESH
        ).wait_send()

    left(X.at[0:3], xsend.at[0])
    left(UB.at[0:7], bsend.at[0])
    for kind in range(len(PIECES)):
        for power in range(5):
            left(some(kind, power), wsend.at[kind * 5 + power])
    left(D.at[:, :, :, :, :, pl.ds(0, 128)], sibs.at[0])
    left(U.at[:, :, :, 0], sibs.at[1])
    for i in range(3):
        left(FP, ysend.at[i])
    pltpu.make_async_copy(O, out, stored.at[0]).wait()


def on_device(patch_tokens, norm_gain, norm_bias, up_weight, up_bias, down_weight, down_bias):
    hbm = pl.BlockSpec(memory_space=pltpu.HBM)
    vmem = pl.BlockSpec(memory_space=pltpu.VMEM)
    dma = pltpu.SemaphoreType.DMA
    return pl.pallas_call(
        kernel,
        out_shape=jax.ShapeDtypeStruct((128, 4096), BF16),
        in_specs=[hbm, vmem, vmem, hbm, hbm, hbm, vmem],
        out_specs=hbm,
        scratch_shapes=[
            pltpu.VMEM((4, 128, 1024), BF16),
            pltpu.VMEM((512, 1024), BF16),
            pltpu.VMEM((4, 4, 2, 2, 64, 512), BF16),
            pltpu.VMEM((8, 1, 512), F32),
            pltpu.VMEM((2, 4, 2, 4, 512, 256), BF16),
            pltpu.VMEM((512, 2048), BF16),
            pltpu.VMEM((128, 4096), BF16),
            pltpu.VMEM((16, 128, 256), F32),
            pltpu.VMEM((16, 128, 256), F32),
            *[pltpu.VMEM((16, 128, 256), BF16)] * 6,
            dma((5,)),
            dma((5 * len(PIECES),)),
            dma((len(ARRIVALS),)),
            dma((1,)),
            dma((3,)),
            dma((1,)),
            dma((8,)),
            dma((2,)),
            dma((24,)),
            dma((3,)),
            dma((32,)),
            dma((1,)),
        ],
        compiler_params=pltpu.CompilerParams(
            collective_id=0, has_side_effects=True, vmem_limit_bytes=62 * 1024 * 1024
        ),
    )(
        patch_tokens,
        norm_gain.reshape(1, -1),
        norm_bias.reshape(1, -1),
        up_weight,
        up_bias.reshape(1, -1),
        down_weight,
        down_bias.reshape(1, -1),
    )


def solution(mesh):
    return jax.shard_map(
        on_device,
        mesh=mesh,
        in_specs=(P(("img", "tp"), None), P(), P(), P("img", "tp"), P("tp"), P("tp", "img"), P()),
        out_specs=P(("img", "tp"), None),
        check_vma=False,
    )
```

```python
import jax
import jax.numpy as jnp
from jax import lax
from jax.experimental import pallas as pl
from jax.experimental.pallas import tpu as pltpu
from jax.sharding import PartitionSpec as P

MESH = pl.DeviceIdType.MESH
F32, BF16 = jnp.float32, jnp.bfloat16

WAIT, SEND, SHARE_U, SHARE_D, NORM, HIDDEN, PART, DIRECT, RELAY, FINAL, LAST = range(11)
XP, XQ, YP, YQ, ZP, ZQ = range(6)
TOK, SIB_U, SIB_D, FAR = range(-4, 0)

WUA, WUB, D0, D0B, D1, D1B = range(6)
PIECES = ((None, 0, 32), (None, 32, 32), (0, 0, 384), (0, 384, 128), (1, 0, 256), (1, 256, 256))
BIASED = WUB
FROM_X = (WUA, D0,)

STEPS = (
    (SEND, XP, WUA, 0, 0), (SEND, XQ, WUA, 0, 0), (SEND, YP, TOK, 0), (SEND, YQ, TOK, 0), (SEND, ZP, WUA, 0, 0),
    (SEND, ZQ, WUA, 0, 0), (SEND, XP, D0, 0, 0), (SEND, XQ, WUB, 0, 0), (SEND, ZP, WUB, 0, 0), (SEND, ZQ, WUB, 0, 0),
    (SEND, XQ, D0, 0, 0), (SEND, ZP, D1, 0, 0), (SEND, ZQ, D1, 0, 0), (SEND, XP, D0B, 0, 0), (SEND, ZP, D1B, 0, 0),
    (SEND, ZQ, D1B, 0, 0), (SEND, XP, WUB, 0, 0), (SEND, XQ, D0B, 0, 0), (WAIT, WUA, -1, 0), (WAIT, WUA, 1, 0),
    (SEND, ZP, WUA, 1, 0), (SEND, ZQ, WUA, 1, 0), (SEND, ZP, WUA, -1, 0), (SEND, ZQ, WUA, -1, 0), (WAIT, WUA, 0, -1),
    (WAIT, WUA, 0, 1), (WAIT, WUB, 0, -1), (SEND, XP, WUB, 0, -1), (SEND, XQ, WUB, 0, -1), (SEND, ZP, WUB, 0, -1),
    (SEND, ZP, WUA, 0, -1), (WAIT, WUB, 0, 1), (SEND, XP, WUB, 0, 1), (SEND, XQ, WUB, 0, 1), (SEND, XP, WUA, -1, 0),
    (SEND, ZQ, WUB, 0, 1), (SEND, ZQ, WUA, 0, 1), (WAIT, D0, -1, 0), (WAIT, D1, 0, -1), (SEND, XQ, D1, 0, -1),
    (SEND, XP, D1, 0, -1), (SEND, ZP, D1, 0, -1), (WAIT, D1, 0, 1), (SEND, XQ, D1, 0, 1), (SEND, ZQ, D1, 0, 1),
    (WAIT, D0B, -1, 0), (WAIT, D0, 1, 0), (WAIT, WUB, -1, 0), (WAIT, D1B, 0, -1), (SEND, XQ, D1B, 0, -1),
    (WAIT, D1B, 0, 1), (WAIT, WUB, -1, -1), (SEND, XP, WUB, -1, -1), (WAIT, WUA, 1, -1), (SEND, ZP, WUA, 1, -1),
    (WAIT, WUA, 1, 1), (SEND, ZQ, WUA, 1, 1), (WAIT, WUB, -1, 1), (SEND, XP, WUB, -1, 1), (SEND, XP, WUB, -1, 0),
    (WAIT, TOK, -1), (SEND, YP, TOK, -1), (WAIT, TOK, 1), (WAIT, WUA, -1, -1), (WAIT, WUA, -1, 1), (WAIT, WUA, 2, 0),
    (WAIT, WUB, 0, -2), (SEND, ZP, WUB, 0, -2), (SEND, XP, WUB, 0, -2), (SEND, XQ, WUB, 0, -2), (WAIT, WUB, 0, 2),
    (SEND, ZQ, WUB, 0, 2), (SEND, XP, WUB, 0, 2), (SEND, XQ, WUB, 0, 2), (SEND, XP, D1, 0, 1), (SEND, XQ, D1B, 0, 1),
    (WAIT, WUA, 0, -2), (SEND, ZP, WUA, 0, -2), (SEND, ZP, WUA, 2, 0), (SEND, ZP, WUA, -1, -1), (WAIT, WUA, 0, 2),
    (SEND, ZQ, WUA, 0, 2), (SEND, ZQ, WUA, 2, 0), (SEND, ZQ, WUA, -1, 1), (WAIT, D1, -1, -1), (WAIT, D1, 0, -2),
    (WAIT, D1, 0, 2), (WAIT, WUA, 1, -2), (SEND, ZP, WUA, 1, -2), (WAIT, WUA, 1, 2), (SEND, ZQ, WUA, 1, 2),
    (SEND, ZQ, D1B, 0, 1), (SEND, ZQ, D1, 0, 2), (WAIT, WUB, 0, -3), (SEND, XP, WUB, 0, -3), (SEND, XQ, WUB, 0, -3),
    (SEND, ZP, WUB, 0, -3), (WAIT, WUB, 0, 3), (SEND, XQ, WUB, 0, 3), (SEND, XQ, D1, 0, 0), (SEND, XQ, D1B, 0, 0),
    (SHARE_U, 0), (WAIT, WUB, -1, -2), (SEND, XP, WUB, -1, -2), (SEND, XP, WUB, 0, 3), (WAIT, WUA, 0, -3),
    (SEND, ZP, WUA, 0, -3), (SEND, ZP, D1B, 0, -1), (WAIT, WUA, 0, 3), (WAIT, TOK, 2), (NORM,), (WAIT, WUB, -1, 2),
    (SEND, XP, WUB, -1, 2), (SEND, XP, D1B, 0, -1), (WAIT, WUA, 2, -1), (WAIT, WUA, 2, 1), (WAIT, SIB_U, 0),
    (WAIT, WUA, -1, -2), (SEND, ZP, WUA, -1, -2), (WAIT, WUA, -1, 2), (SEND, ZQ, WUA, -1, 2), (SEND, ZQ, WUA, 2, 1),
    (SHARE_U, -1), (SHARE_U, 1), (WAIT, D1, -1, 1), (WAIT, WUA, 1, -3), (SEND, ZP, WUA, 1, -3),
    (SEND, ZP, WUA, 2, -1), (SEND, ZP, D1, 0, -2), (WAIT, WUA, 1, 3), (WAIT, WUB, -1, -3), (SEND, XP, WUB, -1, -3),
    (WAIT, WUB, 0, -4), (SEND, XQ, WUB, 0, -4), (SEND, XQ, D1, 0, -2), (WAIT, WUA, 0, -4), (WAIT, D1B, 0, 2),
    (SEND, ZQ, D1B, 0, 2), (SEND, ZQ, D0, 0, 0), (WAIT, SIB_U, 1), (WAIT, WUB, -1, 3), (SEND, XP, WUB, -1, 3),
    (SEND, XP, WUB, 0, -4), (SEND, XP, D1B, 0, 1), (WAIT, SIB_U, -1), (HIDDEN, 0), (WAIT, D1B, 0, -2),
    (WAIT, D1, 0, 3), (SEND, XQ, D1, 0, 3), (SEND, XP, D1, 0, 3), (SEND, XQ, D1, 0, 2), (WAIT, WUA, -1, -3),
    (SEND, ZP, WUA, -1, -3), (SEND, ZP, D1B, 0, -2), (WAIT, WUA, -1, 3), (WAIT, D1B, -1, -1), (WAIT, WUA, 1, -4),
    (WAIT, WUA, 2, 2), (SEND, ZQ, WUA, 2, 2), (SEND, ZQ, D0B, 0, 0), (SEND, ZQ, D0, 1, 0), (SHARE_U, 2),
    (WAIT, WUA, 2, -2), (SEND, ZP, WUA, 2, -2), (SHARE_U, -2), (WAIT, D1B, 0, 3), (SEND, XQ, D1B, 0, 3),
    (WAIT, SIB_U, -2), (WAIT, WUB, -1, -4), (SEND, XP, WUB, -1, -4), (SEND, XP, D1B, 0, 3), (WAIT, D1, 0, -3),
    (SEND, ZP, D1, 0, -3), (SEND, XQ, D1, 0, -3), (SEND, ZP, D0, 0, 0), (SEND, XP, D1, 0, -3), (WAIT, SIB_U, 2),
    (HIDDEN, 1), (WAIT, WUA, -1, -4), (WAIT, D1B, -1, 1), (WAIT, D0, 0, 1), (SEND, ZQ, D0, 0, 1), (WAIT, D1B, 0, -3),
    (SEND, XP, D1B, 0, -3), (SEND, XP, D1, 0, 0), (SEND, XP, D1B, 0, 0), (WAIT, WUA, 2, 3), (SHARE_D, 1, 0, 1),
    (SHARE_U, 3), (WAIT, D1, -1, 3), (WAIT, WUA, 2, -3), (SEND, ZP, WUA, 2, -3), (SEND, ZP, D1B, 0, -3),
    (SEND, ZP, D0B, 0, 0), (WAIT, D0B, 0, 1), (SEND, XQ, D0B, 0, 1), (SEND, XQ, D1B, 0, -3), (SEND, ZQ, D0B, 0, 1),
    (SEND, XQ, D1B, 0, 2), (SEND, XQ, D1B, 0, -2), (SHARE_U, -3), (WAIT, D1, 0, -4), (WAIT, SIB_D, 1, 0, 1),
    (WAIT, D1B, -1, 3), (WAIT, D0, 1, 1), (SEND, ZQ, D0, 1, 1), (WAIT, SIB_U, 3), (WAIT, SIB_U, -3), (HIDDEN, 2),
    (WAIT, D1, -1, -3), (WAIT, D0, 0, -1), (SEND, ZP, D0, 0, -1), (SEND, ZP, D0, 1, 0), (WAIT, WUA, 2, -4),
    (WAIT, D0, 0, 2), (SEND, ZQ, D0, 0, 2), (SHARE_U, -4), (WAIT, D1B, -1, -3), (WAIT, D0B, 0, 2),
    (SEND, XQ, D0B, 0, 2), (SEND, XP, D0B, 0, 2), (SEND, XP, D1, 0, -2), (SEND, XQ, D1, 0, -4),
    (SEND, ZQ, D0B, 0, 2), (SEND, XP, D1, 0, 2), (SEND, XP, D1B, 0, 2), (SEND, XP, D1B, 0, -2),
    (SEND, XP, D1, 0, -4), (SHARE_D, 1, -1, 1), (SHARE_D, 1, 1, 1), (WAIT, D1B, 0, -4), (SHARE_D, 1, 0, 0),
    (WAIT, SIB_U, -4), (HIDDEN, 3), (WAIT, D1, -1, 0), (WAIT, D0B, 0, -1), (SEND, XQ, D0B, 0, -1),
    (SEND, XQ, D1B, 0, -4), (SEND, ZP, D0B, 0, -1), (SEND, ZP, D0, -1, 0), (WAIT, D0, 1, 2), (SEND, ZQ, D0, 1, 2),
    (SEND, ZQ, D0, -1, 0), (PART, 1, 0, 1), (WAIT, SIB_D, 1, 1, 1), (WAIT, D1B, -1, 0), (PART, 1, 1, 1),
    (WAIT, SIB_D, 1, -1, 1), (WAIT, D0B, -1, 2), (WAIT, D0, 0, -2), (SEND, ZP, D0, 0, -2), (WAIT, D0, 0, 3),
    (PART, 1, -1, 1), (WAIT, SIB_D, 1, 0, 0), (WAIT, D1, -1, -2), (WAIT, D0B, 0, 3), (SEND, XQ, D0B, 0, 3),
    (PART, 1, 0, 0), (WAIT, D0, 1, -1), (WAIT, D1, -1, 2), (WAIT, D0B, 0, -2), (SEND, XQ, D0B, 0, -2),
    (SEND, XP, D0B, 0, -2), (SEND, ZP, D0B, 0, -2), (SEND, XP, D1B, 0, -4), (SEND, ZP, D0, 1, -1),
    (SEND, XP, D0B, 0, 1), (SEND, XP, D0B, 0, -1), (SEND, XP, D0B, 0, 3), (SEND, XP, D0, -1, 0),
    (WAIT, FAR, 1, 0, 1), (WAIT, D0, 1, 3), (SHARE_D, 1, 1, 0), (RELAY, 1, 0, 1), (WAIT, D1B, -1, 2),
    (WAIT, FAR, 1, 1, 1), (WAIT, D0, -1, -1), (SEND, ZP, D0, -1, -1), (WAIT, D1B, -1, -2), (RELAY, 1, 1, 1),
    (WAIT, D0, -1, 1), (SEND, ZQ, D0, -1, 1), (WAIT, SIB_D, 1, -1, 0), (WAIT, D1, -1, -4), (WAIT, FAR, 1, -1, 1),
    (WAIT, D0, 0, -3), (SEND, ZP, D0, 0, -3), (WAIT, D0B, -1, -2), (RELAY, 1, -1, 1), (WAIT, D0B, 0, -3),
    (SEND, XQ, D0B, 0, -3), (SEND, XP, D0B, 0, -3), (SEND, XP, D0B, -1, 0), (SEND, XP, D0B, -1, 2),
    (SEND, XP, D0B, -1, -2), (SEND, ZP, D0B, 0, -3), (SEND, XP, D1, -1, -1), (SEND, XP, D1, -1, 1),
    (SEND, XP, D1B, -1, -1), (SEND, XP, D1B, -1, 1), (SHARE_D, 0, 0, 1), (WAIT, D1B, -1, -4), (SHARE_D, 1, -1, 0),
    (PART, 1, -1, 0), (WAIT, D0B, -1, 1), (WAIT, FAR, 1, 0, 0), (WAIT, D0, 1, -2), (SEND, ZP, D0, 1, -2),
    (WAIT, D0B, -1, -1), (WAIT, D0B, -1, 3), (RELAY, 1, 0, 0), (FINAL, 1, 0, 1), (FINAL, 1, 1, 1),
    (WAIT, SIB_D, 0, 0, 1), (PART, 0, 0, 1), (WAIT, D0, 2, 0), (SEND, ZP, D0, 2, 0), (SEND, ZQ, D0, 2, 0),
    (WAIT, D0, -1, -2), (SEND, ZP, D0, -1, -2), (WAIT, D0B, -1, -3), (WAIT, SIB_D, 1, 1, 0), (WAIT, D0, -1, 2),
    (SEND, ZQ, D0, -1, 2), (PART, 1, 1, 0), (WAIT, D0, 0, -4), (WAIT, D0B, 0, -4), (SEND, XQ, D0B, 0, -4),
    (SEND, XP, D0B, 0, -4), (SEND, XP, D1, -1, 3), (SEND, XP, D1B, -1, 3), (SEND, XP, D1, -1, -3),
    (SEND, XP, D1B, -1, -3), (SEND, XP, D1, -1, 0), (SHARE_D, 0, 0, 0), (FINAL, 1, -1, 1), (WAIT, FAR, 1, -1, 0),
    (RELAY, 1, -1, 0), (WAIT, D0, 1, -3), (SEND, ZP, D0, 1, -3), (SHARE_D, 0, 1, 1), (FINAL, 1, 0, 0),
    (WAIT, SIB_D, 0, 0, 0), (WAIT, FAR, 0, 0, 1), (RELAY, 0, 0, 1), (PART, 0, 0, 0), (WAIT, D0B, -1, -4),
    (SEND, XP, D0B, -1, -4), (SEND, XP, D1B, -1, 0), (SEND, XP, D1, -1, -2), (SEND, XP, D1, -1, 2),
    (SEND, XP, D1B, -1, 2), (SEND, XP, D1B, -1, -2), (SEND, XP, D1, -1, -4), (SEND, XP, D1B, -1, -4),
    (SEND, XP, D0B, -1, 1), (SEND, XP, D0B, -1, -1), (SEND, XP, D0B, -1, 3), (SEND, XP, D0B, -1, -3),
    (WAIT, D0, 2, -1), (SEND, ZP, D0, 2, -1), (WAIT, D0, 2, 1), (SEND, ZQ, D0, 2, 1), (WAIT, SIB_D, 0, -1, 1),
    (WAIT, FAR, 1, 1, 0), (RELAY, 1, 1, 0), (FINAL, 1, -1, 0), (WAIT, D0, -1, -3), (SEND, ZP, D0, -1, -3),
    (WAIT, D0, -1, 3), (SHARE_D, 0, -1, 1), (PART, 0, -1, 1), (SHARE_D, 1, 2, 1), (FINAL, 0, 0, 1),
    (WAIT, D0, 1, -4), (SHARE_D, 0, 1, 0), (WAIT, FAR, 0, 0, 0), (RELAY, 0, 0, 0), (WAIT, SIB_D, 0, 1, 1),
    (PART, 0, 1, 1), (WAIT, D0, 2, 2), (SEND, ZQ, D0, 2, 2), (WAIT, D0, 2, -2), (SEND, ZP, D0, 2, -2),
    (WAIT, SIB_D, 1, 2, 1), (PART, 1, 2, 1), (WAIT, D0, -1, -4), (SHARE_D, 0, -1, 0), (FINAL, 1, 1, 0),
    (WAIT, SIB_D, 0, -1, 0), (WAIT, FAR, 0, -1, 1), (RELAY, 0, -1, 1), (PART, 0, -1, 0), (FINAL, 0, 0, 0),
    (SHARE_D, 1, 2, 0), (WAIT, SIB_D, 0, 1, 0), (PART, 0, 1, 0), (WAIT, FAR, 0, 1, 1), (WAIT, D0, 2, 3),
    (WAIT, D0, 2, -3), (SEND, ZP, D0, 2, -3), (RELAY, 0, 1, 1), (SHARE_D, 0, 2, 1), (WAIT, FAR, 1, 2, 1),
    (RELAY, 1, 2, 1), (WAIT, SIB_D, 1, 2, 0), (PART, 1, 2, 0), (WAIT, FAR, 0, -1, 0), (RELAY, 0, -1, 0),
    (WAIT, SIB_D, 0, 2, 1), (PART, 0, 2, 1), (WAIT, D0, 2, -4), (SHARE_D, 0, 2, 0), (FINAL, 0, -1, 1),
    (WAIT, FAR, 0, 1, 0), (RELAY, 0, 1, 0), (FINAL, 0, 1, 1), (WAIT, SIB_D, 0, 2, 0), (DIRECT, 0, 2, 0),
    (WAIT, FAR, 1, 2, 0), (RELAY, 1, 2, 0), (WAIT, FAR, 0, 2, 1), (RELAY, 0, 2, 1), (FINAL, 1, 2, 1),
    (FINAL, 0, -1, 0), (FINAL, 0, 1, 0), (LAST, 0, 2, 0), (FINAL, 1, 2, 0), (FINAL, 0, 2, 1),
)

ITEMS = [(h, dx, rp) for h in (0, 1) for dx in (0, -1, 1, 2) for rp in (0, 1)]
OFFSETS = (0, -1, 1, -2, 2, -3, 3, -4)
AFTER = {XP: -1, XQ: 1, YP: -1, YQ: 1, ZP: -1, ZQ: 1}


def slot(dx):
    return dx % 4


def piece_index(kind, dx, dz):
    if kind in FROM_X or slot(dx) in (0, 3):
        return kind * 32 + slot(dx) * 8 + dz % 8
    if PIECES[kind][0] is None:
        return kind * 32 + 8 + dz % 8
    return kind * 32 + slot(dx) * 8 + dz % 2


def piece_semaphore(kind, dx, dz):
    return ARRIVALS.index(piece_index(kind, dx, dz))


ARRIVALS = sorted({piece_index(k, dx, dz) for k in range(len(PIECES)) for dx in (0, -1, 1, 2) for dz in OFFSETS if dx or dz})


def kernel(
    tok, gain_in, nbias_in, up, upb, down, dbias_in, out,
    gain, nbias, dbias, X, N, U, UB, D, H, A0, A1, S1, S2, S3, RL, FP, FQ,
    loc, wsend, wrecv, xsend, xrecv, bsend, brecv, sibs, sibr, ysend, yrecv,
):
    img, tp = lax.axis_index("img"), lax.axis_index("tp")
    c = lax.rem(img, 2)
    zlo = lax.rem(img // 2, 2)
    x = img // 4
    zhi = lax.rem(tp, 4)
    y = tp // 4
    z = zhi * 2 + zlo
    sign = 1 - 2 * c

    def wrap(v, n):
        return lax.rem(v + 2 * n, n)

    def at(dx=0, dy=0, dz=0, core=None):
        xx, yy, zz = wrap(x + sign * dx, 4), wrap(y + sign * dy, 4), wrap(z + sign * dz, 8)
        cc = c if core is None else core
        return {"img": xx * 4 + lax.rem(zz, 2) * 2 + cc, "tp": yy * 4 + zz // 2}

    sibling = at(core=1 - c)
    opposite = at(dy=2)
    link = {
        XP: at(dx=1), XQ: at(dx=-1), YP: at(dy=1), YQ: at(dy=-1), ZP: at(dz=1), ZQ: at(dz=-1),
    }

    copies = [
        pltpu.make_async_copy(tok, X.at[0], loc.at[0]),
        pltpu.make_async_copy(up, U.at[zhi, x, zlo, c], loc.at[1]),
        pltpu.make_async_copy(down.at[:, pl.ds(0, 128)], D.at[0, 0, 0, zhi, :, pl.ds(0, 128)], loc.at[2]),
        pltpu.make_async_copy(down.at[:, pl.ds(128, 128)], D.at[1, 0, 0, zhi, :, pl.ds(0, 128)], loc.at[3]),
        pltpu.make_async_copy(upb, UB.at[z], loc.at[4]),
    ]
    late = [
        pltpu.make_async_copy(src, dst, loc.at[5 + i])
        for i, (src, dst) in enumerate(((gain_in, gain), (nbias_in, nbias), (dbias_in, dbias)))
    ]
    for copy in copies + late:
        copy.start()
    barrier = pltpu.get_barrier_semaphore()
    partners = [sibling, *link.values(), opposite]
    for device in partners:
        pl.semaphore_signal(barrier, inc=1, device_id=device, device_id_type=MESH)
    pl.semaphore_wait(barrier, len(partners))
    for copy in copies:
        copy.wait()

    def send(src, dst, ssem, rsem, device):
        pltpu.make_async_remote_copy(
            src_ref=src, dst_ref=dst, send_sem=ssem, recv_sem=rsem, device_id=device, device_id_type=MESH
        ).start()

    def arrive(ref, rsem):
        pltpu.make_async_remote_copy(
            src_ref=ref, dst_ref=ref, send_sem=rsem, recv_sem=rsem, device_id=sibling, device_id_type=MESH
        ).wait_recv()

    def where(kind, dx, dz, dx_there=None, dz_there=None):
        half, row, rows = PIECES[kind]
        zz = wrap(z + sign * dz, 8)
        if half is None:
            return U.at[zz // 2, wrap(x + sign * dx, 4), lax.rem(zz, 2), c, pl.ds(row, rows)]
        dx_there = dx if dx_there is None else dx_there
        dz_there = dz if dz_there is None else dz_there
        return D.at[half, slot(dx_there), dz_there % 2, zz // 2, pl.ds(row, rows), pl.ds(0, 128)]

    def some(kind, power):
        half, _, rows = PIECES[kind]
        if half is None:
            whole = U.at[:, :, :, :, pl.ds(0, rows)]
            return (whole.at[0, 0, 0, 0], whole.at[0, 0, 0], whole.at[0, 0], whole.at[0, 0:2], whole.at[0])[power]
        whole = D.at[:, :, :, :, pl.ds(0, rows), pl.ds(0, 128)]
        return (whole.at[0, 0, 0, 0], whole.at[0, 0, 0, 0:2], whole.at[0, 0, 0], whole.at[0, 0], whole.at[0, 0:2])[power]

    sent = [0] * len(PIECES)
    used = [0]

    def forward(path, kind, dx, dz):
        step = AFTER[path]
        dx_there, dz_there = (dx + step, dz) if path in (XP, XQ) else (dx, dz + step)
        send(
            where(kind, dx, dz),
            where(kind, dx, dz, dx_there, dz_there),
            wsend.at[kind * 5 + (sent[kind] + 1).bit_length() - 1],
            wrecv.at[piece_semaphore(kind, dx_there, dz_there)],
            link[path],
        )
        sent[kind] += 1
        if kind == BIASED and path in (ZP, ZQ):
            bias = UB.at[wrap(z + sign * dz, 8)]
            send(bias, bias, bsend.at[0], brecv.at[dz_there % 8], link[path])

    def forward_tokens(path, dy):
        there = slot(dy + AFTER[path])
        send(X.at[slot(dy)], X.at[there], xsend.at[0], xrecv.at[there - 1], link[path])

    def send_y(src, dst, rsem, device):
        send(src, dst, ysend.at[used[0] // 16], rsem, device)
        used[0] += 1

    for step in STEPS:
        op, args = step[0], step[1:]
        if op == SEND:
            if args[1] == TOK:
                forward_tokens(args[0], args[2])
            else:
                forward(*args)
        elif op == WAIT:
            kind = args[0]
            if kind == TOK:
                arrive(X.at[slot(args[1])], xrecv.at[slot(args[1]) - 1])
            elif kind >= 0:
                arrive(where(*args), wrecv.at[piece_semaphore(*args)])
                if kind == BIASED and args[1] == 0:
                    arrive(UB.at[wrap(z + sign * args[2], 8)], brecv.at[args[2] % 8])
            elif kind == SIB_U:
                zz = wrap(z + sign * args[1], 8)
                arrive(U.at[zz // 2, :, lax.rem(zz, 2), 1 - c], sibr.at[16 + args[1] % 8])
            elif kind == SIB_D:
                h, dx, rp = args[1:]
                arrive(D.at[h, slot(dx), rp, :, :, pl.ds(128, 128)], sibr.at[ITEMS.index((h, dx, rp))])
            else:
                i = ITEMS.index(args[1:])
                arrive(RL.at[i], yrecv.at[i])
        elif op == SHARE_U:
            dz = args[0]
            zz = wrap(z + sign * dz, 8)
            block = U.at[zz // 2, :, lax.rem(zz, 2), c]
            for kind, (half, _, _) in enumerate(PIECES):
                if half is None and kind not in FROM_X:
                    arrive(some(kind, 1), wrecv.at[piece_semaphore(kind, 1, dz)])
            send(block, block, sibs.at[1], sibr.at[16 + (-dz) % 8], sibling)
        elif op == SHARE_D:
            h, dx, rp = args
            there = ITEMS.index((h, -dx if dx in (-1, 1) else dx, rp))
            for kind, (half, _, _) in enumerate(PIECES):
                if half == h and kind not in FROM_X and dx in (1, 2):
                    arrive(some(kind, 2), wrecv.at[piece_semaphore(kind, dx, rp)])
            send(
                D.at[h, slot(dx), rp, :, :, pl.ds(0, 128)],
                D.at[h, slot(-dx), rp, :, :, pl.ds(128, 128)],
                sibs.at[0],
                sibr.at[there],
                sibling,
            )
        elif op == NORM:
            for copy in late:
                copy.wait()

            @pl.loop(0, 4)
            def _(r):
                values = X[r].astype(F32)
                center = jnp.mean(values, axis=1, keepdims=True)
                spread = jnp.mean((values - center) ** 2, axis=1, keepdims=True)
                rows = (values - center) * lax.rsqrt(spread + 1e-05) * gain[...] + nbias[...]
                N[pl.ds(pl.multiple_of(r * 128, 128), 128), :] = rows.astype(BF16)

        elif op == HIDDEN:
            side = 1 - 2 * zlo
            zz = wrap(z + (0, -2 * side, 2 * side, 4)[args[0]], 8)
            g = zz // 2
            summed = jnp.dot(N[...], U[g].reshape(1024, 512), preferred_element_type=F32)
            hidden = jax.nn.gelu(summed + UB[zz], approximate=True)
            H[:, pl.ds(pl.multiple_of(g * 512, 512), 512)] = hidden.astype(BF16)

        elif op in (PART, DIRECT):
            h, dx, rp = args
            i = ITEMS.index(args)
            columns = D[h, slot(dx), rp].reshape(2048, 256)
            here, there = (jnp.dot(H[m : m + 256], columns, preferred_element_type=F32) for m in (0, 256))
            A0[i] = here[0:128]
            S2[i] = there[0:128].astype(BF16)
            S3[i] = there[128:256].astype(BF16)
            if op == PART:
                A1[i] = here[128:256]
                send_y(S2.at[i], RL.at[i], yrecv.at[i], link[YP])
                send_y(S3.at[i], FP.at[i], yrecv.at[16 + i], link[YQ])
            else:
                S1[i] = here[128:256].astype(BF16)
                send_y(S2.at[i], RL.at[i], yrecv.at[16 + i], opposite)
                send_y(S3.at[i], FP.at[i], yrecv.at[16 + i], link[YQ])
                send_y(S1.at[i], FQ.at[i], yrecv.at[16 + i], link[YP])
        elif op == RELAY:
            i = ITEMS.index(args)
            S1[i] = (A1[i] + RL[i].astype(F32)).astype(BF16)
            send_y(S1.at[i], FQ.at[i], yrecv.at[16 + i], link[YP])
        elif op in (FINAL, LAST):
            h, dx, rp = args
            i = ITEMS.index(args)
            block = wrap(x + sign * dx, 4) * 4 + lax.rem(zlo + rp, 2) * 2
            arrive(FP.at[0 : 2 if op == FINAL else 3], yrecv.at[16 + i])
            total = A0[i] + FP[i].astype(F32) + FQ[i].astype(F32)
            if op == LAST:
                total = total + RL[i].astype(F32)
            for half, core in ((0, c), (1, 1 - c)):
                cols = pl.ds(pl.multiple_of((block + core) * 256 + h * 128, 128), 128)
                out[:, cols] = (total[:, half * 128 : half * 128 + 128] + dbias[:, cols]).astype(BF16)

    def left(ref, ssem):
        pltpu.make_async_remote_copy(
            src_ref=ref, dst_ref=ref, send_sem=ssem, recv_sem=ssem, device_id=sibling, device_id_type=MESH
        ).wait_send()

    left(X.at[0:3], xsend.at[0])
    left(UB.at[0:7], bsend.at[0])
    for kind in range(len(PIECES)):
        for power in range(5):
            left(some(kind, power), wsend.at[kind * 5 + power])
    left(D.at[:, :, :, :, :, pl.ds(0, 128)], sibs.at[0])
    left(U.at[:, :, :, 0], sibs.at[1])
    for i in range(3):
        left(FP, ysend.at[i])


def on_device(patch_tokens, norm_gain, norm_bias, up_weight, up_bias, down_weight, down_bias):
    hbm = pl.BlockSpec(memory_space=pltpu.HBM)
    vmem = pl.BlockSpec(memory_space=pltpu.VMEM)
    dma = pltpu.SemaphoreType.DMA
    return pl.pallas_call(
        kernel,
        out_shape=pltpu.VMEM((128, 4096), BF16),
        in_specs=[hbm] * 7,
        out_specs=vmem,
        scratch_shapes=[
            pltpu.VMEM((1, 1024), F32),
            pltpu.VMEM((1, 1024), F32),
            pltpu.VMEM((1, 4096), F32),
            pltpu.VMEM((4, 128, 1024), BF16),
            pltpu.VMEM((512, 1024), BF16),
            pltpu.VMEM((4, 4, 2, 2, 64, 512), BF16),
            pltpu.VMEM((8, 1, 512), F32),
            pltpu.VMEM((2, 4, 2, 4, 512, 256), BF16),
            pltpu.VMEM((512, 2048), BF16),
            pltpu.VMEM((16, 128, 256), F32),
            pltpu.VMEM((16, 128, 256), F32),
            *[pltpu.VMEM((16, 128, 256), BF16)] * 6,
            dma((8,)),
            dma((5 * len(PIECES),)),
            dma((len(ARRIVALS),)),
            dma((1,)),
            dma((3,)),
            dma((1,)),
            dma((8,)),
            dma((2,)),
            dma((24,)),
            dma((3,)),
            dma((32,)),
        ],
        compiler_params=pltpu.CompilerParams(
            collective_id=0, has_side_effects=True, vmem_limit_bytes=62 * 1024 * 1024
        ),
    )(
        *(
            pltpu.with_memory_space_constraint(v, pltpu.HBM)
            for v in (
                patch_tokens,
                norm_gain.reshape(1, -1),
                norm_bias.reshape(1, -1),
                up_weight,
                up_bias.reshape(1, -1),
                down_weight,
                down_bias.reshape(1, -1),
            )
        )
    )


def solution(mesh):
    return jax.shard_map(
        on_device,
        mesh=mesh,
        in_specs=(P(("img", "tp"), None), P(), P(), P("img", "tp"), P("tp"), P("tp", "img"), P()),
        out_specs=P(("img", "tp"), None),
        check_vma=False,
    )
```

```python
import jax
import jax.numpy as jnp
from jax import lax
from jax.experimental import pallas as pl
from jax.experimental.pallas import tpu as pltpu
from jax.sharding import PartitionSpec as P

MESH = pl.DeviceIdType.MESH
F32, BF16 = jnp.float32, jnp.bfloat16

WAIT, SEND, SHARE_U, SHARE_D, NORM, HIDDEN, PART, DIRECT, RELAY, FINAL, LAST = range(11)
XP, XQ, YP, YQ, ZP, ZQ = range(6)
TOK, SIB_D, FAR = range(-3, 0)

WUA, WUB, D0, D0B, D1, D1B = range(6)
PIECES = ((None, 0, 32), (None, 32, 32), (0, 0, 384), (0, 384, 128), (1, 0, 256), (1, 256, 256))
BIASED = WUB
FROM_X = (WUA, D0,)

STEPS = (
    (SEND, XP, WUA, 0, 0), (SEND, XQ, WUA, 0, 0), (SEND, YP, TOK, 0), (SEND, YQ, TOK, 0), (SEND, ZP, WUA, 0, 0),
    (SEND, ZQ, WUA, 0, 0), (SEND, XP, D0B, 0, 0), (SEND, XQ, WUB, 0, 0), (SEND, ZP, WUB, 0, 0),
    (SEND, ZQ, WUB, 0, 0), (SEND, XP, D0, 0, 0), (SEND, XQ, D0, 0, 0), (SEND, ZP, D1, 0, 0), (SEND, ZQ, D1, 0, 0),
    (SEND, ZP, D1B, 0, 0), (SEND, ZQ, D1B, 0, 0), (SEND, XP, WUB, 0, 0), (SEND, XQ, D0B, 0, 0), (WAIT, WUA, -1, 0),
    (WAIT, WUA, 1, 0), (SEND, ZP, WUA, 1, 0), (SEND, ZQ, WUA, 1, 0), (SEND, ZP, WUA, -1, 0), (SEND, ZQ, WUA, -1, 0),
    (WAIT, WUA, 0, -1), (WAIT, WUA, 0, 1), (WAIT, D0B, -1, 0), (WAIT, WUB, 0, -1), (SEND, XP, WUB, 0, -1),
    (SEND, XQ, WUB, 0, -1), (SEND, ZP, WUB, 0, -1), (SEND, ZP, WUA, 0, -1), (WAIT, WUB, 0, 1), (SEND, XP, WUB, 0, 1),
    (SEND, XQ, WUB, 0, 1), (SEND, XP, WUA, -1, 0), (SEND, ZQ, WUB, 0, 1), (SEND, ZQ, WUA, 0, 1), (WAIT, D1, 0, -1),
    (SEND, XQ, D1, 0, -1), (SEND, XP, D1, 0, -1), (SEND, ZP, D1, 0, -1), (WAIT, D1, 0, 1), (SEND, XQ, D1, 0, 1),
    (SEND, ZQ, D1, 0, 1), (WAIT, D0, -1, 0), (WAIT, D0, 1, 0), (WAIT, WUB, -1, 0), (WAIT, D1B, 0, -1),
    (SEND, XQ, D1B, 0, -1), (WAIT, D1B, 0, 1), (WAIT, WUB, -1, -1), (SEND, XP, WUB, -1, -1), (WAIT, WUA, 1, -1),
    (SEND, ZP, WUA, 1, -1), (WAIT, WUA, 1, 1), (SEND, ZQ, WUA, 1, 1), (WAIT, WUB, -1, 1), (SEND, XP, WUB, -1, 1),
    (WAIT, TOK, -1), (SEND, YP, TOK, -1), (WAIT, TOK, 1), (WAIT, WUA, -1, -1), (WAIT, WUA, -1, 1), (WAIT, WUA, 2, 0),
    (WAIT, WUB, 0, -2), (SEND, XP, WUB, 0, -2), (SEND, ZP, WUB, 0, -2), (SEND, XQ, WUB, 0, -2), (WAIT, WUB, 0, 2),
    (SEND, ZQ, WUB, 0, 2), (SEND, XP, WUB, 0, 2), (SEND, XP, WUB, -1, 0), (SEND, XQ, WUB, 0, 2),
    (SEND, XP, D1, 0, 1), (SEND, XQ, D1B, 0, 1), (WAIT, WUA, 0, -2), (SEND, ZP, WUA, 0, -2), (SEND, ZP, WUA, 2, 0),
    (SEND, ZP, WUA, -1, -1), (WAIT, WUA, 0, 2), (SEND, ZQ, WUA, 0, 2), (SEND, ZQ, WUA, 2, 0), (SEND, ZQ, WUA, -1, 1),
    (WAIT, D1, -1, -1), (WAIT, D1, 0, -2), (WAIT, D1, 0, 2), (WAIT, WUA, 1, -2), (SEND, ZP, WUA, 1, -2),
    (WAIT, WUA, 1, 2), (SEND, ZQ, WUA, 1, 2), (SEND, ZQ, D1B, 0, 1), (SEND, ZQ, D1, 0, 2), (WAIT, WUB, -1, -2),
    (WAIT, WUB, 0, -3), (SEND, XP, WUB, 0, -3), (SEND, XQ, WUB, 0, -3), (SEND, ZP, WUB, 0, -3), (WAIT, WUB, 0, 3),
    (SEND, XQ, WUB, 0, 3), (SEND, XP, WUB, 0, 3), (SEND, XP, WUB, -1, -2), (SEND, XQ, D1B, 0, 0),
    (SEND, XQ, D1, 0, -2), (WAIT, WUB, -1, 2), (SEND, XP, WUB, -1, 2), (SEND, XP, D1B, 0, -1), (WAIT, WUA, 0, -3),
    (SEND, ZP, WUA, 0, -3), (SEND, ZP, D1B, 0, -1), (WAIT, WUA, 0, 3), (WAIT, TOK, 2), (NORM,), (WAIT, WUA, 2, -1),
    (WAIT, WUA, 2, 1), (WAIT, WUA, -1, -2), (SEND, ZP, WUA, -1, -2), (WAIT, WUA, -1, 2), (SEND, ZQ, WUA, -1, 2),
    (SEND, ZQ, WUA, 2, 1), (SHARE_U, 0), (SHARE_U, -1), (SHARE_U, 1), (WAIT, D1, -1, 1), (WAIT, WUA, 1, -3),
    (SEND, ZP, WUA, 1, -3), (SEND, ZP, WUA, 2, -1), (SEND, ZP, D1, 0, -2), (WAIT, WUA, 1, 3), (WAIT, WUB, -1, -3),
    (SEND, XP, WUB, -1, -3), (WAIT, WUB, 0, -4), (SEND, XQ, WUB, 0, -4), (SEND, XQ, D1, 0, 2), (WAIT, WUB, -1, 3),
    (SEND, XP, WUB, -1, 3), (SEND, XP, WUB, 0, -4), (WAIT, WUA, 0, -4), (WAIT, D1B, 0, 2), (SEND, ZQ, D1B, 0, 2),
    (SEND, ZQ, D0, 0, 0), (SEND, XP, D1B, 0, 2), (SEND, XP, D1B, 0, 1), (HIDDEN, 0), (WAIT, D1B, 0, -2),
    (WAIT, D1, 0, 3), (SEND, XQ, D1, 0, 3), (SEND, XQ, D1B, 0, -2), (WAIT, WUA, -1, -3), (SEND, ZP, WUA, -1, -3),
    (SEND, ZP, D1B, 0, -2), (WAIT, WUA, -1, 3), (WAIT, D1B, -1, -1), (WAIT, WUA, 1, -4), (WAIT, WUA, 2, 2),
    (SEND, ZQ, WUA, 2, 2), (SEND, ZQ, D0B, 0, 0), (SEND, ZQ, D0, 1, 0), (SHARE_U, 2), (WAIT, WUA, 2, -2),
    (SEND, ZP, WUA, 2, -2), (SHARE_U, -2), (WAIT, D1B, 0, 3), (SEND, XQ, D1B, 0, 3), (WAIT, WUB, -1, -4),
    (SEND, XP, WUB, -1, -4), (SEND, XP, D1, 0, 3), (SEND, XP, D1B, 0, 3), (WAIT, D1, 0, -3), (SEND, ZP, D1, 0, -3),
    (SEND, XQ, D1, 0, -3), (SEND, ZP, D0, 0, 0), (SEND, XP, D1, 0, -3), (HIDDEN, 1), (WAIT, WUA, -1, -4),
    (WAIT, D1B, -1, 2), (WAIT, D0, 0, 1), (SEND, ZQ, D0, 0, 1), (WAIT, D1B, 0, -3), (SEND, XQ, D1B, 0, -3),
    (SEND, XP, D1B, 0, -3), (SEND, XP, D1, 0, 0), (WAIT, WUA, 2, 3), (SHARE_D, 1, 0, 1), (SHARE_U, 3),
    (WAIT, D1B, -1, 1), (WAIT, WUA, 2, -3), (SEND, ZP, WUA, 2, -3), (SEND, ZP, D1B, 0, -3), (SEND, ZP, D0B, 0, 0),
    (WAIT, D0B, 0, 1), (SEND, ZQ, D0B, 0, 1), (SHARE_U, -3), (WAIT, D1, 0, -4), (SEND, XQ, D1, 0, -4),
    (SEND, XQ, D0B, 0, 1), (SEND, XQ, D1B, 0, 2), (WAIT, SIB_D, 1, 0, 1), (WAIT, D1, -1, 3), (WAIT, D0, 1, 1),
    (SEND, ZQ, D0, 1, 1), (HIDDEN, 2), (WAIT, D1B, -1, 3), (WAIT, D0, 0, -1), (SEND, ZP, D0, 0, -1),
    (SEND, ZP, D0, 1, 0), (WAIT, WUA, 2, -4), (WAIT, D0, 0, 2), (SEND, ZQ, D0, 0, 2), (SHARE_D, 1, 1, 1),
    (SHARE_U, -4), (WAIT, D1, -1, -3), (WAIT, D0B, 0, 2), (SEND, XQ, D0B, 0, 2), (SEND, XP, D0B, 0, 2),
    (SEND, XP, D1B, 0, 0), (SEND, ZQ, D0B, 0, 2), (SEND, XP, D1, 0, -2), (SEND, XP, D1, 0, 2),
    (SEND, XP, D1B, 0, -2), (SEND, XP, D1, 0, -4), (WAIT, D1B, 0, -4), (SEND, XQ, D1B, 0, -4),
    (SEND, XP, D1B, 0, -4), (SHARE_D, 1, 0, 0), (WAIT, D1B, -1, -3), (WAIT, D0B, 0, -1), (SEND, XQ, D0B, 0, -1),
    (SEND, XQ, D1, 0, 0), (SEND, ZP, D0B, 0, -1), (SEND, ZP, D0, -1, 0), (SHARE_D, 1, -1, 1),
    (WAIT, SIB_D, 1, -1, 1), (WAIT, D0, 1, 2), (SEND, ZQ, D0, 1, 2), (SEND, ZQ, D0, -1, 0), (HIDDEN, 3),
    (WAIT, D1, -1, 0), (WAIT, SIB_D, 1, 0, 0), (PART, 1, 0, 1), (WAIT, D0B, -1, 2), (WAIT, D0, 0, -2),
    (SEND, ZP, D0, 0, -2), (WAIT, SIB_D, 1, 1, 1), (PART, 1, -1, 1), (WAIT, D1B, -1, 0), (WAIT, D0B, 0, 3),
    (SEND, XQ, D0B, 0, 3), (PART, 1, 0, 0), (WAIT, D0, 1, -1), (SEND, ZP, D0, 1, -1), (PART, 1, 1, 1),
    (WAIT, D1, -1, -2), (WAIT, D0B, 0, -2), (SEND, XQ, D0B, 0, -2), (SEND, XP, D0B, 0, -2), (SEND, XP, D0B, 0, 1),
    (SEND, ZP, D0B, 0, -2), (SEND, XP, D0B, 0, -1), (SEND, XP, D0B, -1, 0), (SEND, XP, D0, -1, 0),
    (SEND, XP, D0B, 0, 3), (SEND, XP, D1, -1, -1), (SHARE_D, 1, 1, 0), (WAIT, D1, -1, 2), (WAIT, FAR, 1, 0, 1),
    (RELAY, 1, 0, 1), (WAIT, D0, -1, -1), (SEND, ZP, D0, -1, -1), (WAIT, D1B, -1, -2), (WAIT, D0, -1, 1),
    (SEND, ZQ, D0, -1, 1), (WAIT, D1, -1, -4), (WAIT, FAR, 1, -1, 1), (RELAY, 1, -1, 1), (WAIT, SIB_D, 1, -1, 0),
    (WAIT, D0, 0, -3), (SEND, ZP, D0, 0, -3), (WAIT, D1B, -1, -4), (SHARE_D, 1, -1, 0), (PART, 1, -1, 0),
    (WAIT, D0B, -1, -2), (WAIT, FAR, 1, 0, 0), (WAIT, D0, 1, -2), (WAIT, D0B, -1, 1), (WAIT, D0B, 0, -3),
    (SEND, XP, D0B, 0, -3), (SEND, XQ, D0B, 0, -3), (SEND, ZP, D0B, 0, -3), (SEND, XP, D1, -1, 1),
    (SEND, ZP, D0, 1, -2), (SEND, XP, D1B, -1, -1), (SEND, XP, D1B, -1, 1), (SEND, XP, D1, -1, 3),
    (WAIT, D0B, -1, -1), (SHARE_D, 0, 0, 1), (RELAY, 1, 0, 0), (WAIT, FAR, 1, 1, 1), (RELAY, 1, 1, 1),
    (WAIT, SIB_D, 1, 1, 0), (WAIT, D0, 2, 0), (SEND, ZQ, D0, 2, 0), (PART, 1, 1, 0), (WAIT, D0B, -1, 3),
    (WAIT, D0, -1, -2), (SEND, ZP, D0, -1, -2), (SEND, ZP, D0, 2, 0), (WAIT, D0, -1, 2), (SEND, ZQ, D0, -1, 2),
    (WAIT, SIB_D, 0, 0, 1), (PART, 0, 0, 1), (WAIT, D0B, -1, -3), (WAIT, D0B, 0, -4), (SEND, XQ, D0B, 0, -4),
    (SEND, XP, D0B, 0, -4), (SEND, XP, D1B, -1, 3), (SEND, XP, D1, -1, -3), (SEND, XP, D1B, -1, -3),
    (SEND, XP, D0B, -1, 2), (SEND, XP, D0B, -1, -2), (SEND, XP, D1, -1, 0), (SEND, XP, D1B, -1, 0),
    (SEND, XP, D1B, -1, 2), (SEND, XP, D1, -1, -2), (SEND, XP, D1, -1, 2), (SEND, XP, D1B, -1, -2),
    (SEND, XP, D1, -1, -4), (SEND, XP, D1B, -1, -4), (SHARE_D, 0, 0, 0), (FINAL, 1, 0, 1), (WAIT, FAR, 1, -1, 0),
    (RELAY, 1, -1, 0), (FINAL, 1, -1, 1), (FINAL, 1, 0, 0), (WAIT, D0, 1, -3), (SEND, ZP, D0, 1, -3),
    (SHARE_D, 0, 1, 1), (FINAL, 1, 1, 1), (WAIT, SIB_D, 0, 0, 0), (WAIT, D0, 2, 1), (SEND, ZQ, D0, 2, 1),
    (PART, 0, 0, 0), (WAIT, D0B, -1, -4), (SEND, XP, D0B, -1, -4), (SEND, XP, D0B, -1, 1), (SEND, XP, D0B, -1, -1),
    (SEND, XP, D0B, -1, 3), (SEND, XP, D0B, -1, -3), (WAIT, FAR, 1, 1, 0), (RELAY, 1, 1, 0), (WAIT, D0, -1, -3),
    (SEND, ZP, D0, -1, -3), (WAIT, SIB_D, 0, -1, 1), (WAIT, FAR, 0, 0, 1), (RELAY, 0, 0, 1), (SHARE_D, 0, -1, 1),
    (PART, 0, -1, 1), (WAIT, D0, 2, -1), (SEND, ZP, D0, 2, -1), (SHARE_D, 1, 2, 1), (FINAL, 1, -1, 0),
    (WAIT, D0, 2, 2), (SEND, ZQ, D0, 2, 2), (WAIT, SIB_D, 0, 1, 1), (WAIT, FAR, 0, 0, 0), (RELAY, 0, 0, 0),
    (SHARE_D, 0, 1, 0), (PART, 0, 1, 1), (WAIT, SIB_D, 1, 2, 1), (SHARE_D, 0, -1, 0), (PART, 1, 2, 1),
    (FINAL, 1, 1, 0), (WAIT, D0, 2, -2), (SEND, ZP, D0, 2, -2), (FINAL, 0, 0, 1), (WAIT, SIB_D, 0, -1, 0),
    (PART, 0, -1, 0), (WAIT, FAR, 0, -1, 1), (WAIT, SIB_D, 0, 1, 0), (RELAY, 0, -1, 1), (PART, 0, 1, 0),
    (SHARE_D, 1, 2, 0), (FINAL, 0, 0, 0), (WAIT, FAR, 0, 1, 1), (RELAY, 0, 1, 1), (WAIT, D0, 2, -3),
    (SEND, ZP, D0, 2, -3), (SHARE_D, 0, 2, 1), (WAIT, FAR, 1, 2, 1), (RELAY, 1, 2, 1), (WAIT, SIB_D, 1, 2, 0),
    (PART, 1, 2, 0), (WAIT, FAR, 0, -1, 0), (RELAY, 0, -1, 0), (WAIT, SIB_D, 0, 2, 1), (PART, 0, 2, 1),
    (WAIT, FAR, 0, 1, 0), (SHARE_D, 0, 2, 0), (RELAY, 0, 1, 0), (FINAL, 0, -1, 1), (FINAL, 0, 1, 1),
    (WAIT, SIB_D, 0, 2, 0), (WAIT, FAR, 1, 2, 0), (RELAY, 1, 2, 0), (DIRECT, 0, 2, 0), (WAIT, FAR, 0, 2, 1),
    (RELAY, 0, 2, 1), (FINAL, 1, 2, 1), (FINAL, 0, -1, 0), (FINAL, 0, 1, 0), (FINAL, 1, 2, 0), (LAST, 0, 2, 0),
    (FINAL, 0, 2, 1),
)

ITEMS = [(h, dx, rp) for h in (0, 1) for dx in (0, -1, 1, 2) for rp in (0, 1)]
OFFSETS = (0, -1, 1, -2, 2, -3, 3, -4)
AFTER = {XP: -1, XQ: 1, YP: -1, YQ: 1, ZP: -1, ZQ: 1}


def slot(dx):
    return dx % 4


def rows_of(half, from_x):
    return sum(PIECES[k][2] for k in range(len(PIECES)) if PIECES[k][0] == half and (k in FROM_X) == from_x)


def arrival(kind, dx, dz):
    half, from_x = PIECES[kind][0], kind in FROM_X
    if half is None:
        return (1, kind, dz, 0) if not from_x and dx in (1, 2) else (0, kind, dx, dz)
    if from_x:
        return (3, half, dx, dz) if dz in (3, -4) else (0, kind, dx, dz)
    return (2, half, dx, dz % 2) if dx in (1, 2) else (0, kind, dx, dz)


ARRIVALS = sorted({arrival(k, dx, dz) for k in range(len(PIECES)) for dx in (0, -1, 1, 2) for dz in OFFSETS if dx or dz})

SIZES = sorted({(half is None, rows) for half, _, rows in PIECES})
GROUPS = [
    (size, power)
    for size in SIZES
    for power in range(7)
    if 31 * sum((half is None, rows) == size for half, _, rows in PIECES) >> power & 1
]
LEAVE = {size: [GROUPS.index((s, p)) for s, p in GROUPS if s == size for _ in range(2**p)] for size in SIZES}


def kernel(
    tok, gain_in, nbias_in, up, upb, down, dbias_in, out,
    gain, nbias, dbias, X, N, U, UB, D, H, A0, A1, S1, S2, S3, RL, FP, FQ,
    loc, wsend, wrecv, xsend, xrecv, bsend, brecv, sibs, sibr, ysend, yrecv,
):
    img, tp = lax.axis_index("img"), lax.axis_index("tp")
    c = lax.rem(img, 2)
    zlo = lax.rem(img // 2, 2)
    x = img // 4
    zhi = lax.rem(tp, 4)
    y = tp // 4
    z = zhi * 2 + zlo
    sign = 1 - 2 * c

    def wrap(v, n):
        return lax.rem(v + 2 * n, n)

    def at(dx=0, dy=0, dz=0, core=None):
        xx, yy, zz = wrap(x + sign * dx, 4), wrap(y + sign * dy, 4), wrap(z + sign * dz, 8)
        cc = c if core is None else core
        return {"img": xx * 4 + lax.rem(zz, 2) * 2 + cc, "tp": yy * 4 + zz // 2}

    sibling = at(core=1 - c)
    opposite = at(dy=2)
    link = {
        XP: at(dx=1), XQ: at(dx=-1), YP: at(dy=1), YQ: at(dy=-1), ZP: at(dz=1), ZQ: at(dz=-1),
    }

    copies = [
        pltpu.make_async_copy(tok, X.at[0], loc.at[0]),
        pltpu.make_async_copy(up, U.at[zhi, x, zlo, c], loc.at[1]),
        pltpu.make_async_copy(down.at[:, pl.ds(0, 128)], D.at[0, 0, 0, zhi, :, pl.ds(0, 128)], loc.at[2]),
        pltpu.make_async_copy(down.at[:, pl.ds(128, 128)], D.at[1, 0, 0, zhi, :, pl.ds(0, 128)], loc.at[3]),
        pltpu.make_async_copy(upb, UB.at[z], loc.at[4]),
    ]
    late = [
        pltpu.make_async_copy(src, dst, loc.at[5 + i])
        for i, (src, dst) in enumerate(((gain_in, gain), (nbias_in, nbias), (dbias_in, dbias)))
    ]
    for copy in copies + late:
        copy.start()
    barrier = pltpu.get_barrier_semaphore()
    partners = [sibling, *link.values(), opposite]
    for device in partners:
        pl.semaphore_signal(barrier, inc=1, device_id=device, device_id_type=MESH)
    pl.semaphore_wait(barrier, len(partners))
    for copy in copies:
        copy.wait()

    def send(src, dst, ssem, rsem, device):
        pltpu.make_async_remote_copy(
            src_ref=src, dst_ref=dst, send_sem=ssem, recv_sem=rsem, device_id=device, device_id_type=MESH
        ).start()

    def arrive(ref, rsem):
        pltpu.make_async_remote_copy(
            src_ref=ref, dst_ref=ref, send_sem=rsem, recv_sem=rsem, device_id=sibling, device_id_type=MESH
        ).wait_recv()

    def where(kind, dx, dz, dx_there=None, dz_there=None):
        half, row, rows = PIECES[kind]
        zz = wrap(z + sign * dz, 8)
        if half is None:
            return U.at[zz // 2, wrap(x + sign * dx, 4), lax.rem(zz, 2), c, pl.ds(row, rows)]
        dx_there = dx if dx_there is None else dx_there
        dz_there = dz if dz_there is None else dz_there
        return D.at[half, slot(dx_there), dz_there % 2, zz // 2, pl.ds(row, rows), pl.ds(0, 128)]

    def some(size, power):
        if size[0]:
            v = U.at[:, :, :, :, pl.ds(0, size[1])]
            return (v.at[0, 0, 0, 0], v.at[0, 0, 0], v.at[0, 0], v.at[0, 0:2], v.at[0], v.at[0:2], v)[power]
        v = D.at[:, :, :, :, pl.ds(0, size[1]), pl.ds(0, 128)]
        return (v.at[0, 0, 0, 0], v.at[0, 0, 0, 0:2], v.at[0, 0, 0], v.at[0, 0], v.at[0, 0:2], v.at[0], v)[power]

    leaving = {size: list(groups) for size, groups in LEAVE.items()}
    used = [0]

    def forward(path, kind, dx, dz):
        step = AFTER[path]
        dx_there, dz_there = (dx + step, dz) if path in (XP, XQ) else (dx, dz + step)
        dx_there = 2 if dx_there == -2 else dx_there
        send(
            where(kind, dx, dz),
            where(kind, dx, dz, dx_there, dz_there),
            wsend.at[leaving[(PIECES[kind][0] is None, PIECES[kind][2])].pop()],
            wrecv.at[ARRIVALS.index(arrival(kind, dx_there, dz_there))],
            link[path],
        )
        if kind == BIASED and path in (ZP, ZQ):
            bias = UB.at[wrap(z + sign * dz, 8)]
            send(bias, bias, bsend.at[0], brecv.at[dz_there % 8], link[path])

    def forward_tokens(path, dy):
        there = slot(dy + AFTER[path])
        send(X.at[slot(dy)], X.at[there], xsend.at[0], xrecv.at[there - 1], link[path])

    def send_y(src, dst, rsem, device):
        send(src, dst, ysend.at[used[0] // 16], rsem, device)
        used[0] += 1

    for step in STEPS:
        op, args = step[0], step[1:]
        if op == SEND:
            if args[1] == TOK:
                forward_tokens(args[0], args[2])
            else:
                forward(*args)
        elif op == WAIT:
            kind = args[0]
            if kind == TOK:
                arrive(X.at[slot(args[1])], xrecv.at[slot(args[1]) - 1])
            elif kind >= 0:
                arrive(where(*args), wrecv.at[ARRIVALS.index(arrival(*args))])
                if kind == BIASED and args[1] == 0:
                    arrive(UB.at[wrap(z + sign * args[2], 8)], brecv.at[args[2] % 8])
            elif kind == SIB_D:
                h, dx, rp = args[1:]
                arrive(D.at[h, slot(dx), rp, :, :, pl.ds(128, 128)], sibr.at[ITEMS.index((h, dx, rp))])
            else:
                i = ITEMS.index(args[1:])
                arrive(RL.at[i], yrecv.at[i])
        elif op == SHARE_U:
            dz = args[0]
            zz = wrap(z + sign * dz, 8)
            block = U.at[zz // 2, :, lax.rem(zz, 2), c]
            for kind, (half, _, _) in enumerate(PIECES):
                if half is None and kind not in FROM_X:
                    arrive(some((True, PIECES[kind][2]), 1), wrecv.at[ARRIVALS.index(arrival(kind, 1, dz))])
            send(block, block, sibs.at[1], sibr.at[16 + max(abs(dz) - 1, 0)], sibling)
        elif op == SHARE_D:
            h, dx, rp = args
            there = ITEMS.index((h, -dx if dx in (-1, 1) else dx, rp))
            if rows_of(h, False) and dx in (1, 2):
                block = D.at[0, 0, 0, :, pl.ds(0, rows_of(h, False)), pl.ds(0, 128)]
                arrive(block, wrecv.at[ARRIVALS.index((2, h, dx, rp))])
            if rows_of(h, True):
                block = D.at[0, 0, 0, 0, pl.ds(0, rows_of(h, True)), pl.ds(0, 128)]
                arrive(block, wrecv.at[ARRIVALS.index((3, h, dx, 3 if rp else -4))])
            send(
                D.at[h, slot(dx), rp, :, :, pl.ds(0, 128)],
                D.at[h, slot(-dx), rp, :, :, pl.ds(128, 128)],
                sibs.at[0],
                sibr.at[there],
                sibling,
            )
        elif op == NORM:
            for copy in late:
                copy.wait()

            @pl.loop(0, 4)
            def _(r):
                values = X[r].astype(F32)
                center = jnp.mean(values, axis=1, keepdims=True)
                spread = jnp.mean((values - center) ** 2, axis=1, keepdims=True)
                rows = (values - center) * lax.rsqrt(spread + 1e-05) * gain[...] + nbias[...]
                N[pl.ds(pl.multiple_of(r * 128, 128), 128), :] = rows.astype(BF16)

        elif op == HIDDEN:
            arrive(U.at[0 : (3, 2, 2, 1)[args[0]], :, 0, 0], sibr.at[16 + args[0]])
            side = 1 - 2 * zlo
            zz = wrap(z + (0, -2 * side, 2 * side, 4)[args[0]], 8)
            g = zz // 2
            summed = jnp.dot(N[...], U[g].reshape(1024, 512), preferred_element_type=F32)
            hidden = jax.nn.gelu(summed + UB[zz], approximate=True)
            H[:, pl.ds(pl.multiple_of(g * 512, 512), 512)] = hidden.astype(BF16)

        elif op in (PART, DIRECT):
            h, dx, rp = args
            i = ITEMS.index(args)
            columns = D[h, slot(dx), rp].reshape(2048, 256)
            here, there = (jnp.dot(H[m : m + 256], columns, preferred_element_type=F32) for m in (0, 256))
            A0[i] = here[0:128]
            S2[i] = there[0:128].astype(BF16)
            S3[i] = there[128:256].astype(BF16)
            if op == PART:
                A1[i] = here[128:256]
                send_y(S2.at[i], RL.at[i], yrecv.at[i], link[YP])
                send_y(S3.at[i], FP.at[i], yrecv.at[16 + i], link[YQ])
            else:
                S1[i] = here[128:256].astype(BF16)
                send_y(S2.at[i], RL.at[i], yrecv.at[16 + i], opposite)
                send_y(S3.at[i], FP.at[i], yrecv.at[16 + i], link[YQ])
                send_y(S1.at[i], FQ.at[i], yrecv.at[16 + i], link[YP])
        elif op == RELAY:
            i = ITEMS.index(args)
            S1[i] = (A1[i] + RL[i].astype(F32)).astype(BF16)
            send_y(S1.at[i], FQ.at[i], yrecv.at[16 + i], link[YP])
        elif op in (FINAL, LAST):
            h, dx, rp = args
            i = ITEMS.index(args)
            block = wrap(x + sign * dx, 4) * 4 + lax.rem(zlo + rp, 2) * 2
            arrive(FP.at[0 : 2 if op == FINAL else 3], yrecv.at[16 + i])
            total = A0[i] + FP[i].astype(F32) + FQ[i].astype(F32)
            if op == LAST:
                total = total + RL[i].astype(F32)
            for half, core in ((0, c), (1, 1 - c)):
                cols = pl.ds(pl.multiple_of((block + core) * 256 + h * 128, 128), 128)
                out[:, cols] = (total[:, half * 128 : half * 128 + 128] + dbias[:, cols]).astype(BF16)

    def left(ref, ssem):
        pltpu.make_async_remote_copy(
            src_ref=ref, dst_ref=ref, send_sem=ssem, recv_sem=ssem, device_id=sibling, device_id_type=MESH
        ).wait_send()

    left(X.at[0:3], xsend.at[0])
    left(UB.at[0:7], bsend.at[0])
    for i, group in enumerate(GROUPS):
        left(some(*group), wsend.at[i])
    left(D.at[:, :, :, :, :, pl.ds(0, 128)], sibs.at[0])
    left(U.at[:, :, :, 0], sibs.at[1])
    for i in range(3):
        left(FP, ysend.at[i])


def on_device(patch_tokens, norm_gain, norm_bias, up_weight, up_bias, down_weight, down_bias):
    hbm = pl.BlockSpec(memory_space=pltpu.HBM)
    vmem = pl.BlockSpec(memory_space=pltpu.VMEM)
    dma = pltpu.SemaphoreType.DMA
    return pl.pallas_call(
        kernel,
        out_shape=pltpu.VMEM((128, 4096), BF16),
        in_specs=[hbm] * 7,
        out_specs=vmem,
        scratch_shapes=[
            pltpu.VMEM((1, 1024), F32),
            pltpu.VMEM((1, 1024), F32),
            pltpu.VMEM((1, 4096), F32),
            pltpu.VMEM((4, 128, 1024), BF16),
            pltpu.VMEM((512, 1024), BF16),
            pltpu.VMEM((4, 4, 2, 2, 64, 512), BF16),
            pltpu.VMEM((8, 1, 512), F32),
            pltpu.VMEM((2, 4, 2, 4, 512, 256), BF16),
            pltpu.VMEM((512, 2048), BF16),
            pltpu.VMEM((16, 128, 256), F32),
            pltpu.VMEM((16, 128, 256), F32),
            *[pltpu.VMEM((16, 128, 256), BF16)] * 6,
            dma((8,)),
            dma((len(GROUPS),)),
            dma((len(ARRIVALS),)),
            dma((1,)),
            dma((3,)),
            dma((1,)),
            dma((8,)),
            dma((2,)),
            dma((20,)),
            dma((3,)),
            dma((32,)),
        ],
        compiler_params=pltpu.CompilerParams(
            collective_id=0, has_side_effects=True, vmem_limit_bytes=62 * 1024 * 1024
        ),
    )(
        *(
            pltpu.with_memory_space_constraint(v, pltpu.HBM)
            for v in (
                patch_tokens,
                norm_gain.reshape(1, -1),
                norm_bias.reshape(1, -1),
                up_weight,
                up_bias.reshape(1, -1),
                down_weight,
                down_bias.reshape(1, -1),
            )
        )
    )


def solution(mesh):
    return jax.shard_map(
        on_device,
        mesh=mesh,
        in_specs=(P(("img", "tp"), None), P(), P(), P("img", "tp"), P("tp"), P("tp", "img"), P()),
        out_specs=P(("img", "tp"), None),
        check_vma=False,
    )
```

```python
import jax
import jax.numpy as jnp
from jax import lax
from jax.experimental import pallas as pl
from jax.experimental.pallas import tpu as pltpu
from jax.sharding import PartitionSpec as P

MESH = pl.DeviceIdType.MESH
F32, BF16 = jnp.float32, jnp.bfloat16

WAIT, SEND, SHARE_U, SHARE_D, NORM, HIDDEN, PART, DIRECT, RELAY, FINAL, LAST = range(11)
XP, XQ, YP, YQ, ZP, ZQ = range(6)
TOK, SIB_D, FAR = range(-3, 0)

WUA, WUB, D0, D0B, D1, D1B = range(6)
PIECES = ((None, 0, 32), (None, 32, 32), (0, 0, 384), (0, 384, 128), (1, 0, 256), (1, 256, 256))
BIASED = WUB
FROM_X = (WUA, D0,)

STEPS = (
    (SEND, XP, WUA, 0, 0), (SEND, XQ, WUA, 0, 0), (SEND, YP, TOK, 0), (SEND, YQ, TOK, 0), (SEND, ZP, WUA, 0, 0),
    (SEND, ZQ, WUA, 0, 0), (SEND, XP, D0B, 0, 0), (SEND, XQ, WUB, 0, 0), (SEND, ZP, WUB, 0, 0),
    (SEND, ZQ, WUB, 0, 0), (SEND, XP, D0, 0, 0), (SEND, XQ, D0, 0, 0), (SEND, ZP, D1, 0, 0), (SEND, ZQ, D1, 0, 0),
    (SEND, ZP, D1B, 0, 0), (SEND, ZQ, D1B, 0, 0), (SEND, XP, WUB, 0, 0), (SEND, XQ, D0B, 0, 0), (WAIT, WUA, -1, 0),
    (WAIT, WUA, 1, 0), (SEND, ZP, WUA, 1, 0), (SEND, ZQ, WUA, 1, 0), (SEND, ZP, WUA, -1, 0), (SEND, ZQ, WUA, -1, 0),
    (WAIT, WUA, 0, -1), (WAIT, WUA, 0, 1), (WAIT, D0B, -1, 0), (WAIT, WUB, 0, -1), (SEND, XP, WUB, 0, -1),
    (SEND, XQ, WUB, 0, -1), (SEND, ZP, WUB, 0, -1), (SEND, ZP, WUA, 0, -1), (WAIT, WUB, 0, 1), (SEND, XP, WUB, 0, 1),
    (SEND, XQ, WUB, 0, 1), (SEND, XP, WUA, -1, 0), (SEND, ZQ, WUB, 0, 1), (SEND, ZQ, WUA, 0, 1), (WAIT, D1, 0, -1),
    (SEND, XQ, D1, 0, -1), (SEND, XP, D1, 0, -1), (SEND, ZP, D1, 0, -1), (WAIT, D1, 0, 1), (SEND, XQ, D1, 0, 1),
    (SEND, ZQ, D1, 0, 1), (WAIT, D0, -1, 0), (WAIT, D0, 1, 0), (WAIT, WUB, -1, 0), (WAIT, D1B, 0, -1),
    (SEND, XQ, D1B, 0, -1), (WAIT, D1B, 0, 1), (WAIT, WUB, -1, -1), (SEND, XP, WUB, -1, -1), (WAIT, WUA, 1, -1),
    (SEND, ZP, WUA, 1, -1), (WAIT, WUA, 1, 1), (SEND, ZQ, WUA, 1, 1), (WAIT, WUB, -1, 1), (SEND, XP, WUB, -1, 1),
    (WAIT, TOK, -1), (SEND, YP, TOK, -1), (WAIT, TOK, 1), (WAIT, WUA, -1, -1), (WAIT, WUA, -1, 1), (WAIT, WUA, 2, 0),
    (WAIT, WUB, 0, -2), (SEND, XP, WUB, 0, -2), (SEND, ZP, WUB, 0, -2), (SEND, XQ, WUB, 0, -2), (WAIT, WUB, 0, 2),
    (SEND, ZQ, WUB, 0, 2), (SEND, XP, WUB, 0, 2), (SEND, XP, WUB, -1, 0), (SEND, XQ, WUB, 0, 2),
    (SEND, XP, D1, 0, 1), (SEND, XQ, D1B, 0, 1), (WAIT, WUA, 0, -2), (SEND, ZP, WUA, 0, -2), (SEND, ZP, WUA, 2, 0),
    (SEND, ZP, WUA, -1, -1), (WAIT, WUA, 0, 2), (SEND, ZQ, WUA, 0, 2), (SEND, ZQ, WUA, 2, 0), (SEND, ZQ, WUA, -1, 1),
    (WAIT, D1, -1, -1), (WAIT, D1, 0, -2), (WAIT, D1, 0, 2), (WAIT, WUA, 1, -2), (SEND, ZP, WUA, 1, -2),
    (WAIT, WUA, 1, 2), (SEND, ZQ, WUA, 1, 2), (SEND, ZQ, D1B, 0, 1), (SEND, ZQ, D1, 0, 2), (WAIT, WUB, -1, -2),
    (WAIT, WUB, 0, -3), (SEND, XP, WUB, 0, -3), (SEND, XQ, WUB, 0, -3), (SEND, ZP, WUB, 0, -3), (WAIT, WUB, 0, 3),
    (SEND, XQ, WUB, 0, 3), (SEND, XP, WUB, 0, 3), (SEND, XP, WUB, -1, -2), (SEND, XQ, D1B, 0, 0),
    (SEND, XQ, D1, 0, -2), (WAIT, WUB, -1, 2), (SEND, XP, WUB, -1, 2), (SEND, XP, D1B, 0, -1), (WAIT, WUA, 0, -3),
    (SEND, ZP, WUA, 0, -3), (SEND, ZP, D1B, 0, -1), (WAIT, WUA, 0, 3), (WAIT, TOK, 2), (NORM,), (WAIT, WUA, 2, -1),
    (WAIT, WUA, 2, 1), (WAIT, WUA, -1, -2), (SEND, ZP, WUA, -1, -2), (WAIT, WUA, -1, 2), (SEND, ZQ, WUA, -1, 2),
    (SEND, ZQ, WUA, 2, 1), (SHARE_U, 0), (SHARE_U, -1), (SHARE_U, 1), (WAIT, D1, -1, 1), (WAIT, WUA, 1, -3),
    (SEND, ZP, WUA, 1, -3), (SEND, ZP, WUA, 2, -1), (SEND, ZP, D1, 0, -2), (WAIT, WUA, 1, 3), (WAIT, WUB, -1, -3),
    (SEND, XP, WUB, -1, -3), (WAIT, WUB, 0, -4), (SEND, XQ, WUB, 0, -4), (SEND, XQ, D1, 0, 2), (WAIT, WUB, -1, 3),
    (SEND, XP, WUB, -1, 3), (SEND, XP, WUB, 0, -4), (WAIT, WUA, 0, -4), (WAIT, D1B, 0, 2), (SEND, ZQ, D1B, 0, 2),
    (SEND, ZQ, D0, 0, 0), (SEND, XP, D1B, 0, 2), (SEND, XP, D1B, 0, 1), (HIDDEN, 0), (WAIT, D1B, 0, -2),
    (WAIT, D1, 0, 3), (SEND, XQ, D1, 0, 3), (SEND, XQ, D1B, 0, -2), (WAIT, WUA, -1, -3), (SEND, ZP, WUA, -1, -3),
    (SEND, ZP, D1B, 0, -2), (WAIT, WUA, -1, 3), (WAIT, D1B, -1, -1), (WAIT, WUA, 1, -4), (WAIT, WUA, 2, 2),
    (SEND, ZQ, WUA, 2, 2), (SEND, ZQ, D0B, 0, 0), (SEND, ZQ, D0, 1, 0), (SHARE_U, 2), (WAIT, WUA, 2, -2),
    (SEND, ZP, WUA, 2, -2), (SHARE_U, -2), (WAIT, D1B, 0, 3), (SEND, XQ, D1B, 0, 3), (WAIT, WUB, -1, -4),
    (SEND, XP, WUB, -1, -4), (SEND, XP, D1, 0, 3), (SEND, XP, D1B, 0, 3), (WAIT, D1, 0, -3), (SEND, ZP, D1, 0, -3),
    (SEND, XQ, D1, 0, -3), (SEND, ZP, D0, 0, 0), (SEND, XP, D1, 0, -3), (HIDDEN, 1), (WAIT, WUA, -1, -4),
    (WAIT, D1B, -1, 2), (WAIT, D0, 0, 1), (SEND, ZQ, D0, 0, 1), (WAIT, D1B, 0, -3), (SEND, XQ, D1B, 0, -3),
    (SEND, XP, D1B, 0, -3), (SEND, XP, D1, 0, 0), (WAIT, WUA, 2, 3), (SHARE_D, 1, 0, 1), (SHARE_U, 3),
    (WAIT, D1B, -1, 1), (WAIT, WUA, 2, -3), (SEND, ZP, WUA, 2, -3), (SEND, ZP, D1B, 0, -3), (SEND, ZP, D0B, 0, 0),
    (WAIT, D0B, 0, 1), (SEND, ZQ, D0B, 0, 1), (SHARE_U, -3), (WAIT, D1, 0, -4), (SEND, XQ, D1, 0, -4),
    (SEND, XQ, D0B, 0, 1), (SEND, XQ, D1B, 0, 2), (WAIT, SIB_D, 1, 0, 1), (WAIT, D1, -1, 3), (WAIT, D0, 1, 1),
    (SEND, ZQ, D0, 1, 1), (HIDDEN, 2), (WAIT, D1B, -1, 3), (WAIT, D0, 0, -1), (SEND, ZP, D0, 0, -1),
    (SEND, ZP, D0, 1, 0), (WAIT, WUA, 2, -4), (WAIT, D0, 0, 2), (SEND, ZQ, D0, 0, 2), (SHARE_D, 1, 1, 1),
    (SHARE_U, -4), (WAIT, D1, -1, -3), (WAIT, D0B, 0, 2), (SEND, XQ, D0B, 0, 2), (SEND, XP, D0B, 0, 2),
    (SEND, XP, D1B, 0, 0), (SEND, ZQ, D0B, 0, 2), (SEND, XP, D1, 0, -2), (SEND, XP, D1, 0, 2),
    (SEND, XP, D1B, 0, -2), (SEND, XP, D1, 0, -4), (WAIT, D1B, 0, -4), (SEND, XQ, D1B, 0, -4),
    (SEND, XP, D1B, 0, -4), (SHARE_D, 1, 0, 0), (WAIT, D1B, -1, -3), (WAIT, D0B, 0, -1), (SEND, XQ, D0B, 0, -1),
    (SEND, XQ, D1, 0, 0), (SEND, ZP, D0B, 0, -1), (SEND, ZP, D0, -1, 0), (SHARE_D, 1, -1, 1),
    (WAIT, SIB_D, 1, -1, 1), (WAIT, D0, 1, 2), (SEND, ZQ, D0, 1, 2), (SEND, ZQ, D0, -1, 0), (HIDDEN, 3),
    (WAIT, D1, -1, 0), (WAIT, SIB_D, 1, 0, 0), (PART, 1, 0, 1), (WAIT, D0B, -1, 2), (WAIT, D0, 0, -2),
    (SEND, ZP, D0, 0, -2), (WAIT, SIB_D, 1, 1, 1), (PART, 1, -1, 1), (WAIT, D1B, -1, 0), (WAIT, D0B, 0, 3),
    (SEND, XQ, D0B, 0, 3), (PART, 1, 0, 0), (WAIT, D0, 1, -1), (SEND, ZP, D0, 1, -1), (PART, 1, 1, 1),
    (WAIT, D1, -1, -2), (WAIT, D0B, 0, -2), (SEND, XQ, D0B, 0, -2), (SEND, XP, D0B, 0, -2), (SEND, XP, D0B, 0, 1),
    (SEND, ZP, D0B, 0, -2), (SEND, XP, D0B, 0, -1), (SEND, XP, D0B, -1, 0), (SEND, XP, D0, -1, 0),
    (SEND, XP, D0B, 0, 3), (SEND, XP, D1, -1, -1), (SHARE_D, 1, 1, 0), (WAIT, D1, -1, 2), (WAIT, FAR, 1, 0, 1),
    (RELAY, 1, 0, 1), (WAIT, D0, -1, -1), (SEND, ZP, D0, -1, -1), (WAIT, D1B, -1, -2), (WAIT, D0, -1, 1),
    (SEND, ZQ, D0, -1, 1), (WAIT, D1, -1, -4), (WAIT, FAR, 1, -1, 1), (RELAY, 1, -1, 1), (WAIT, SIB_D, 1, -1, 0),
    (WAIT, D0, 0, -3), (SEND, ZP, D0, 0, -3), (WAIT, D1B, -1, -4), (SHARE_D, 1, -1, 0), (PART, 1, -1, 0),
    (WAIT, D0B, -1, -2), (WAIT, FAR, 1, 0, 0), (WAIT, D0, 1, -2), (WAIT, D0B, -1, 1), (WAIT, D0B, 0, -3),
    (SEND, XP, D0B, 0, -3), (SEND, XQ, D0B, 0, -3), (SEND, ZP, D0B, 0, -3), (SEND, XP, D1, -1, 1),
    (SEND, ZP, D0, 1, -2), (SEND, XP, D1B, -1, -1), (SEND, XP, D1B, -1, 1), (SEND, XP, D1, -1, 3),
    (WAIT, D0B, -1, -1), (SHARE_D, 0, 0, 1), (RELAY, 1, 0, 0), (WAIT, FAR, 1, 1, 1), (RELAY, 1, 1, 1),
    (WAIT, SIB_D, 1, 1, 0), (WAIT, D0, 2, 0), (SEND, ZQ, D0, 2, 0), (PART, 1, 1, 0), (WAIT, D0B, -1, 3),
    (WAIT, D0, -1, -2), (SEND, ZP, D0, -1, -2), (SEND, ZP, D0, 2, 0), (WAIT, D0, -1, 2), (SEND, ZQ, D0, -1, 2),
    (WAIT, SIB_D, 0, 0, 1), (PART, 0, 0, 1), (WAIT, D0B, -1, -3), (WAIT, D0B, 0, -4), (SEND, XQ, D0B, 0, -4),
    (SEND, XP, D0B, 0, -4), (SEND, XP, D1B, -1, 3), (SEND, XP, D1, -1, -3), (SEND, XP, D1B, -1, -3),
    (SEND, XP, D0B, -1, 2), (SEND, XP, D0B, -1, -2), (SEND, XP, D1, -1, 0), (SEND, XP, D1B, -1, 0),
    (SEND, XP, D1B, -1, 2), (SEND, XP, D1, -1, -2), (SEND, XP, D1, -1, 2), (SEND, XP, D1B, -1, -2),
    (SEND, XP, D1, -1, -4), (SEND, XP, D1B, -1, -4), (SHARE_D, 0, 0, 0), (FINAL, 1, 0, 1), (WAIT, FAR, 1, -1, 0),
    (RELAY, 1, -1, 0), (FINAL, 1, -1, 1), (FINAL, 1, 0, 0), (WAIT, D0, 1, -3), (SEND, ZP, D0, 1, -3),
    (SHARE_D, 0, 1, 1), (FINAL, 1, 1, 1), (WAIT, SIB_D, 0, 0, 0), (WAIT, D0, 2, 1), (SEND, ZQ, D0, 2, 1),
    (PART, 0, 0, 0), (WAIT, D0B, -1, -4), (SEND, XP, D0B, -1, -4), (SEND, XP, D0B, -1, 1), (SEND, XP, D0B, -1, -1),
    (SEND, XP, D0B, -1, 3), (SEND, XP, D0B, -1, -3), (WAIT, FAR, 1, 1, 0), (RELAY, 1, 1, 0), (WAIT, D0, -1, -3),
    (SEND, ZP, D0, -1, -3), (WAIT, SIB_D, 0, -1, 1), (WAIT, FAR, 0, 0, 1), (RELAY, 0, 0, 1), (SHARE_D, 0, -1, 1),
    (PART, 0, -1, 1), (WAIT, D0, 2, -1), (SEND, ZP, D0, 2, -1), (SHARE_D, 1, 2, 1), (FINAL, 1, -1, 0),
    (WAIT, D0, 2, 2), (SEND, ZQ, D0, 2, 2), (WAIT, SIB_D, 0, 1, 1), (WAIT, FAR, 0, 0, 0), (RELAY, 0, 0, 0),
    (SHARE_D, 0, 1, 0), (PART, 0, 1, 1), (WAIT, SIB_D, 1, 2, 1), (SHARE_D, 0, -1, 0), (PART, 1, 2, 1),
    (FINAL, 1, 1, 0), (WAIT, D0, 2, -2), (SEND, ZP, D0, 2, -2), (FINAL, 0, 0, 1), (WAIT, SIB_D, 0, -1, 0),
    (PART, 0, -1, 0), (WAIT, FAR, 0, -1, 1), (WAIT, SIB_D, 0, 1, 0), (RELAY, 0, -1, 1), (PART, 0, 1, 0),
    (SHARE_D, 1, 2, 0), (FINAL, 0, 0, 0), (WAIT, FAR, 0, 1, 1), (RELAY, 0, 1, 1), (WAIT, D0, 2, -3),
    (SEND, ZP, D0, 2, -3), (SHARE_D, 0, 2, 1), (WAIT, FAR, 1, 2, 1), (RELAY, 1, 2, 1), (WAIT, SIB_D, 1, 2, 0),
    (PART, 1, 2, 0), (WAIT, FAR, 0, -1, 0), (RELAY, 0, -1, 0), (WAIT, SIB_D, 0, 2, 1), (PART, 0, 2, 1),
    (WAIT, FAR, 0, 1, 0), (SHARE_D, 0, 2, 0), (RELAY, 0, 1, 0), (FINAL, 0, -1, 1), (FINAL, 0, 1, 1),
    (WAIT, SIB_D, 0, 2, 0), (WAIT, FAR, 1, 2, 0), (RELAY, 1, 2, 0), (DIRECT, 0, 2, 0), (WAIT, FAR, 0, 2, 1),
    (RELAY, 0, 2, 1), (FINAL, 1, 2, 1), (FINAL, 0, -1, 0), (FINAL, 0, 1, 0), (FINAL, 1, 2, 0), (LAST, 0, 2, 0),
    (FINAL, 0, 2, 1),
)

ITEMS = [(h, dx, rp) for h in (0, 1) for dx in (0, -1, 1, 2) for rp in (0, 1)]
OFFSETS = (0, -1, 1, -2, 2, -3, 3, -4)
AFTER = {XP: -1, XQ: 1, YP: -1, YQ: 1, ZP: -1, ZQ: 1}


def slot(dx):
    return dx % 4


def rows_of(half, from_x):
    return sum(PIECES[k][2] for k in range(len(PIECES)) if PIECES[k][0] == half and (k in FROM_X) == from_x)


def arrival(kind, dx, dz):
    half, from_x = PIECES[kind][0], kind in FROM_X
    if half is None:
        return (1, kind, dz, 0) if not from_x and dx in (1, 2) else (0, kind, dx, dz)
    if from_x:
        return (3, half, dx, dz) if dz in (3, -4) else (0, kind, dx, dz)
    return (2, half, dx, dz % 2) if dx in (1, 2) else (0, kind, dx, dz)


ARRIVALS = sorted({arrival(k, dx, dz) for k in range(len(PIECES)) for dx in (0, -1, 1, 2) for dz in OFFSETS if dx or dz})

SIZES = sorted({(half is None, rows) for half, _, rows in PIECES})
GROUPS = [
    (size, power)
    for size in SIZES
    for power in range(7)
    if 31 * sum((half is None, rows) == size for half, _, rows in PIECES) >> power & 1
]
LEAVE = {size: [GROUPS.index((s, p)) for s, p in GROUPS if s == size for _ in range(2**p)] for size in SIZES}


def kernel(
    tok, gain_in, nbias_in, up, upb, down, dbias_in, out,
    gain, nbias, dbias, X, N, U, UB, D, H, A0, A1, S1, S2, S3, RL, FP, FQ,
    loc, wsend, wrecv, xsend, xrecv, bsend, brecv, sibs, sibr, ysend, yrecv,
):
    img, tp = lax.axis_index("img"), lax.axis_index("tp")
    c = lax.rem(img, 2)
    zlo = lax.rem(img // 2, 2)
    x = img // 4
    zhi = lax.rem(tp, 4)
    y = tp // 4
    z = zhi * 2 + zlo
    sign = 1 - 2 * c

    def wrap(v, n):
        return lax.rem(v + 2 * n, n)

    def at(dx=0, dy=0, dz=0, core=None):
        xx, yy, zz = wrap(x + sign * dx, 4), wrap(y + sign * dy, 4), wrap(z + sign * dz, 8)
        cc = c if core is None else core
        return {"img": xx * 4 + lax.rem(zz, 2) * 2 + cc, "tp": yy * 4 + zz // 2}

    sibling = at(core=1 - c)
    opposite = at(dy=2)
    link = {
        XP: at(dx=1), XQ: at(dx=-1), YP: at(dy=1), YQ: at(dy=-1), ZP: at(dz=1), ZQ: at(dz=-1),
    }

    copies = [
        pltpu.make_async_copy(tok, X.at[0], loc.at[0]),
        pltpu.make_async_copy(up, U.at[zhi, x, zlo, c], loc.at[1]),
        pltpu.make_async_copy(down.at[:, pl.ds(0, 128)], D.at[0, 0, 0, zhi, :, pl.ds(0, 128)], loc.at[2]),
        pltpu.make_async_copy(down.at[:, pl.ds(128, 128)], D.at[1, 0, 0, zhi, :, pl.ds(0, 128)], loc.at[3]),
        pltpu.make_async_copy(upb, UB.at[z], loc.at[4]),
    ]
    late = [
        pltpu.make_async_copy(src, dst, loc.at[5 + i])
        for i, (src, dst) in enumerate(((gain_in, gain), (nbias_in, nbias), (dbias_in, dbias)))
    ]
    for copy in copies + late:
        copy.start()
    barrier = pltpu.get_barrier_semaphore()
    partners = [sibling, *link.values(), opposite]
    for device in partners:
        pl.semaphore_signal(barrier, inc=1, device_id=device, device_id_type=MESH)
    pl.semaphore_wait(barrier, len(partners))
    for copy in copies:
        copy.wait()

    def send(src, dst, ssem, rsem, device):
        pltpu.make_async_remote_copy(
            src_ref=src, dst_ref=dst, send_sem=ssem, recv_sem=rsem, device_id=device, device_id_type=MESH
        ).start()

    def arrive(ref, rsem):
        pltpu.make_async_remote_copy(
            src_ref=ref, dst_ref=ref, send_sem=rsem, recv_sem=rsem, device_id=sibling, device_id_type=MESH
        ).wait_recv()

    def where(kind, dx, dz, dx_there=None, dz_there=None):
        half, row, rows = PIECES[kind]
        zz = wrap(z + sign * dz, 8)
        if half is None:
            return U.at[zz // 2, wrap(x + sign * dx, 4), lax.rem(zz, 2), c, pl.ds(row, rows)]
        dx_there = dx if dx_there is None else dx_there
        dz_there = dz if dz_there is None else dz_there
        return D.at[half, slot(dx_there), dz_there % 2, zz // 2, pl.ds(row, rows), pl.ds(0, 128)]

    def some(size, power):
        if size[0]:
            v = U.at[:, :, :, :, pl.ds(0, size[1])]
            return (v.at[0, 0, 0, 0], v.at[0, 0, 0], v.at[0, 0], v.at[0, 0:2], v.at[0], v.at[0:2], v)[power]
        v = D.at[:, :, :, :, pl.ds(0, size[1]), pl.ds(0, 128)]
        return (v.at[0, 0, 0, 0], v.at[0, 0, 0, 0:2], v.at[0, 0, 0], v.at[0, 0], v.at[0, 0:2], v.at[0], v)[power]

    leaving = {size: list(groups) for size, groups in LEAVE.items()}
    used = [0]

    def forward(path, kind, dx, dz):
        step = AFTER[path]
        dx_there, dz_there = (dx + step, dz) if path in (XP, XQ) else (dx, dz + step)
        dx_there = 2 if dx_there == -2 else dx_there
        send(
            where(kind, dx, dz),
            where(kind, dx, dz, dx_there, dz_there),
            wsend.at[leaving[(PIECES[kind][0] is None, PIECES[kind][2])].pop()],
            wrecv.at[ARRIVALS.index(arrival(kind, dx_there, dz_there))],
            link[path],
        )
        if kind == BIASED and path in (ZP, ZQ):
            bias = UB.at[wrap(z + sign * dz, 8)]
            send(bias, bias, bsend.at[0], brecv.at[dz_there % 8], link[path])

    def share(kind, dx, dz):
        half, row, rows = PIECES[kind]
        zz = wrap(z + sign * dz, 8)
        there = (half, -dx if dx in (-1, 1) else dx, dz % 2)
        send(
            D.at[half, slot(dx), dz % 2, zz // 2, pl.ds(row, rows), pl.ds(0, 128)],
            D.at[half, slot(-dx), dz % 2, zz // 2, pl.ds(row, rows), pl.ds(128, 128)],
            sibs.at[0],
            sibr.at[ITEMS.index(there)],
            sibling,
        )

    def forward_tokens(path, dy):
        there = slot(dy + AFTER[path])
        send(X.at[slot(dy)], X.at[there], xsend.at[0], xrecv.at[there - 1], link[path])

    def send_y(src, dst, rsem, device):
        send(src, dst, ysend.at[used[0] // 16], rsem, device)
        used[0] += 1

    for step in STEPS:
        op, args = step[0], step[1:]
        if op == SEND:
            if args[1] == TOK:
                forward_tokens(args[0], args[2])
            else:
                forward(*args)
        elif op == WAIT:
            kind = args[0]
            if kind == TOK:
                arrive(X.at[slot(args[1])], xrecv.at[slot(args[1]) - 1])
            elif kind >= 0:
                arrive(where(*args), wrecv.at[ARRIVALS.index(arrival(*args))])
                if PIECES[kind][0] is not None:
                    share(*args)
                if kind == BIASED and args[1] == 0:
                    arrive(UB.at[wrap(z + sign * args[2], 8)], brecv.at[args[2] % 8])
            elif kind == SIB_D:
                h, dx, rp = args[1:]
                arrive(D.at[h, slot(dx), rp, :, :, pl.ds(128, 128)], sibr.at[ITEMS.index((h, dx, rp))])
            else:
                i = ITEMS.index(args[1:])
                arrive(RL.at[i], yrecv.at[i])
        elif op == SHARE_U:
            dz = args[0]
            zz = wrap(z + sign * dz, 8)
            block = U.at[zz // 2, :, lax.rem(zz, 2), c]
            for kind, (half, _, _) in enumerate(PIECES):
                if half is None and kind not in FROM_X:
                    arrive(some((True, PIECES[kind][2]), 1), wrecv.at[ARRIVALS.index(arrival(kind, 1, dz))])
            send(block, block, sibs.at[1], sibr.at[16 + max(abs(dz) - 1, 0)], sibling)
        elif op == SHARE_D:
            h, dx, rp = args
            if rows_of(h, False) and dx in (1, 2):
                block = D.at[0, 0, 0, :, pl.ds(0, rows_of(h, False)), pl.ds(0, 128)]
                arrive(block, wrecv.at[ARRIVALS.index((2, h, dx, rp))])
            if rows_of(h, True):
                block = D.at[0, 0, 0, 0, pl.ds(0, rows_of(h, True)), pl.ds(0, 128)]
                arrive(block, wrecv.at[ARRIVALS.index((3, h, dx, 3 if rp else -4))])
            for kind, (half, _, _) in enumerate(PIECES):
                if half == h:
                    for dz in OFFSETS:
                        own = dx == 0 and dz == 0
                        if dz % 2 == rp and (own or arrival(kind, dx, dz)[0] != 0):
                            share(kind, dx, dz)
        elif op == NORM:
            for copy in late:
                copy.wait()

            @pl.loop(0, 4)
            def _(r):
                values = X[r].astype(F32)
                center = jnp.mean(values, axis=1, keepdims=True)
                spread = jnp.mean((values - center) ** 2, axis=1, keepdims=True)
                rows = (values - center) * lax.rsqrt(spread + 1e-05) * gain[...] + nbias[...]
                N[pl.ds(pl.multiple_of(r * 128, 128), 128), :] = rows.astype(BF16)

        elif op == HIDDEN:
            arrive(U.at[0 : (3, 2, 2, 1)[args[0]], :, 0, 0], sibr.at[16 + args[0]])
            side = 1 - 2 * zlo
            zz = wrap(z + (0, -2 * side, 2 * side, 4)[args[0]], 8)
            g = zz // 2
            summed = jnp.dot(N[...], U[g].reshape(1024, 512), preferred_element_type=F32)
            hidden = jax.nn.gelu(summed + UB[zz], approximate=True)
            H[:, pl.ds(pl.multiple_of(g * 512, 512), 512)] = hidden.astype(BF16)

        elif op in (PART, DIRECT):
            h, dx, rp = args
            i = ITEMS.index(args)
            columns = D[h, slot(dx), rp].reshape(2048, 256)
            here, there = (jnp.dot(H[m : m + 256], columns, preferred_element_type=F32) for m in (0, 256))
            A0[i] = here[0:128]
            S2[i] = there[0:128].astype(BF16)
            S3[i] = there[128:256].astype(BF16)
            if op == PART:
                A1[i] = here[128:256]
                send_y(S2.at[i], RL.at[i], yrecv.at[i], link[YP])
                send_y(S3.at[i], FP.at[i], yrecv.at[16 + i], link[YQ])
            else:
                S1[i] = here[128:256].astype(BF16)
                send_y(S2.at[i], RL.at[i], yrecv.at[16 + i], opposite)
                send_y(S3.at[i], FP.at[i], yrecv.at[16 + i], link[YQ])
                send_y(S1.at[i], FQ.at[i], yrecv.at[16 + i], link[YP])
        elif op == RELAY:
            i = ITEMS.index(args)
            S1[i] = (A1[i] + RL[i].astype(F32)).astype(BF16)
            send_y(S1.at[i], FQ.at[i], yrecv.at[16 + i], link[YP])
        elif op in (FINAL, LAST):
            h, dx, rp = args
            i = ITEMS.index(args)
            block = wrap(x + sign * dx, 4) * 4 + lax.rem(zlo + rp, 2) * 2
            arrive(FP.at[0 : 2 if op == FINAL else 3], yrecv.at[16 + i])
            total = A0[i] + FP[i].astype(F32) + FQ[i].astype(F32)
            if op == LAST:
                total = total + RL[i].astype(F32)
            for half, core in ((0, c), (1, 1 - c)):
                cols = pl.ds(pl.multiple_of((block + core) * 256 + h * 128, 128), 128)
                out[:, cols] = (total[:, half * 128 : half * 128 + 128] + dbias[:, cols]).astype(BF16)

    def left(ref, ssem):
        pltpu.make_async_remote_copy(
            src_ref=ref, dst_ref=ref, send_sem=ssem, recv_sem=ssem, device_id=sibling, device_id_type=MESH
        ).wait_send()

    left(X.at[0:3], xsend.at[0])
    left(UB.at[0:7], bsend.at[0])
    for i, group in enumerate(GROUPS):
        left(some(*group), wsend.at[i])
    left(D.at[:, :, :, :, :, pl.ds(0, 128)], sibs.at[0])
    left(U.at[:, :, :, 0], sibs.at[1])
    for i in range(3):
        left(FP, ysend.at[i])


def on_device(patch_tokens, norm_gain, norm_bias, up_weight, up_bias, down_weight, down_bias):
    hbm = pl.BlockSpec(memory_space=pltpu.HBM)
    vmem = pl.BlockSpec(memory_space=pltpu.VMEM)
    dma = pltpu.SemaphoreType.DMA
    return pl.pallas_call(
        kernel,
        out_shape=pltpu.VMEM((128, 4096), BF16),
        in_specs=[hbm] * 7,
        out_specs=vmem,
        scratch_shapes=[
            pltpu.VMEM((1, 1024), F32),
            pltpu.VMEM((1, 1024), F32),
            pltpu.VMEM((1, 4096), F32),
            pltpu.VMEM((4, 128, 1024), BF16),
            pltpu.VMEM((512, 1024), BF16),
            pltpu.VMEM((4, 4, 2, 2, 64, 512), BF16),
            pltpu.VMEM((8, 1, 512), F32),
            pltpu.VMEM((2, 4, 2, 4, 512, 256), BF16),
            pltpu.VMEM((512, 2048), BF16),
            pltpu.VMEM((16, 128, 256), F32),
            pltpu.VMEM((16, 128, 256), F32),
            *[pltpu.VMEM((16, 128, 256), BF16)] * 6,
            dma((8,)),
            dma((len(GROUPS),)),
            dma((len(ARRIVALS),)),
            dma((1,)),
            dma((3,)),
            dma((1,)),
            dma((8,)),
            dma((2,)),
            dma((20,)),
            dma((3,)),
            dma((32,)),
        ],
        compiler_params=pltpu.CompilerParams(
            collective_id=0, has_side_effects=True, vmem_limit_bytes=62 * 1024 * 1024
        ),
    )(
        *(
            pltpu.with_memory_space_constraint(v, pltpu.HBM)
            for v in (
                patch_tokens,
                norm_gain.reshape(1, -1),
                norm_bias.reshape(1, -1),
                up_weight,
                up_bias.reshape(1, -1),
                down_weight,
                down_bias.reshape(1, -1),
            )
        )
    )


def solution(mesh):
    return jax.shard_map(
        on_device,
        mesh=mesh,
        in_specs=(P(("img", "tp"), None), P(), P(), P("img", "tp"), P("tp"), P("tp", "img"), P()),
        out_specs=P(("img", "tp"), None),
        check_vma=False,
    )
```
